32 devices in a mesh: batch: 2 (over x), w: 4 (over z), h: 4 (over y, core).
Axes of the slice: x: 2, y: 2, z: 4, core: 2. Of those that a mesh axis runs over, the one named last changes fastest.
Arguments:
- image: bfloat16 [384, 1024, 32, 1], P('batch', 'h', 'w'), parts along dimension 0
- down_w1: bfloat16 [3, 3, 1, 64], replicated
- down_v1: float32 [3, 64], replicated
- refine_w1: bfloat16 [3, 3, 64, 64], replicated
- refine_v1: float32 [3, 64], replicated
- down_w2: bfloat16 [3, 3, 64, 128], replicated
- down_v2: float32 [3, 128], replicated
- refine_w2: bfloat16 [3, 3, 128, 128], replicated
- refine_v2: float32 [3, 128], replicated
- down_w3: bfloat16 [3, 3, 128, 256], replicated
- down_v3: float32 [3, 256], replicated
- refine_w3: bfloat16 [3, 3, 256, 256], replicated
- refine_v3: float32 [3, 256], replicated
Outputs:
- output: bfloat16 [384, 128, 4, 256], P('batch', 'h', 'w'), parts along dimension 0
There are 2 independent parts. The reference program is written for one: setup_inputs(seed, part) draws one part's arguments, and reference() takes and returns one part's arrays. A program takes and returns all parts, laid end to end along the dimension named above; an argument that names none is the same for every part.
All inputs are finite; a program needn't handle non-finite values.
Results may differ from the reference program's by a relative error of at most 0.00397023.
Values are sent between devices in bfloat16 or wider.
A program may use at most 1 GiB of HBM per device.

```python
import jax
import jax.numpy as jnp
from jax import lax

IMAGES = 192
IMG_HEIGHT = 1024
IMG_WIDTH = 32
CHAN_IN = 1
CHAN_ONE = 64
GROUPS = 8
NORM_EPS = 1e-5


def draw_affine(key, channels):
    bias_key, scale_key, shift_key = jax.random.split(key, 3)
    bias = 0.5 * jax.random.normal(bias_key, (channels,), jnp.float32)
    scale = 1.0 + 0.3 * jax.random.normal(scale_key, (channels,), jnp.float32)
    shift = 0.3 * jax.random.normal(shift_key, (channels,), jnp.float32)
    return jnp.stack([bias, scale, shift])


def setup_inputs(seed: int = 0, part: int = 0) -> dict:
    shared_key, image_root = jax.random.split(jax.random.key(seed))
    image_key = jax.random.fold_in(image_root, part)
    noise_key, slope_key, level_key = jax.random.split(image_key, 3)
    noise = jax.random.normal(noise_key, (IMAGES, IMG_HEIGHT, IMG_WIDTH, CHAN_IN), jnp.float32)
    slopes = jax.random.normal(slope_key, (2, IMAGES, 1, 1, CHAN_IN), jnp.float32)
    levels = 0.5 * jax.random.normal(level_key, (IMAGES, 1, 1, CHAN_IN), jnp.float32)
    row_pos = (jnp.arange(IMG_HEIGHT, dtype=jnp.float32) + 0.5) * (2.0 / IMG_HEIGHT) - 1.0
    col_pos = (jnp.arange(IMG_WIDTH, dtype=jnp.float32) + 0.5) * (2.0 / IMG_WIDTH) - 1.0
    ramp = slopes[0] * row_pos[:, None, None] + slopes[1] * col_pos[:, None]
    image = (noise + 1.5 * ramp + levels).astype(jnp.bfloat16)
    widths = [CHAN_IN, CHAN_ONE, 2 * CHAN_ONE, 4 * CHAN_ONE]
    weight_keys = jax.random.split(shared_key, 12)
    inputs = {"image": image}
    for stage in range(3):
        chan_prev = widths[stage]
        chan_next = widths[stage + 1]
        down_w = jax.random.normal(weight_keys[4 * stage], (3, 3, chan_prev, chan_next), jnp.float32) * (9 * chan_prev) ** -0.5
        refine_w = jax.random.normal(weight_keys[4 * stage + 2], (3, 3, chan_next, chan_next), jnp.float32) * (9 * chan_next) ** -0.5
        inputs["down_w" + str(stage + 1)] = down_w.astype(jnp.bfloat16)
        inputs["down_v" + str(stage + 1)] = draw_affine(weight_keys[4 * stage + 1], chan_next)
        inputs["refine_w" + str(stage + 1)] = refine_w.astype(jnp.bfloat16)
        inputs["refine_v" + str(stage + 1)] = draw_affine(weight_keys[4 * stage + 3], chan_next)
    return inputs


def conv_norm(inputs, kernel, affine, stride):
    summed = lax.conv_general_dilated(inputs.astype(jnp.float32), kernel.astype(jnp.float32), (stride, stride), ((1, 1), (1, 1)), dimension_numbers=("NHWC", "HWIO", "NHWC")) + affine[0]
    out_shape = summed.shape
    grouped = summed.reshape(out_shape[0], out_shape[1], out_shape[2], GROUPS, out_shape[3] // GROUPS)
    grp_mean = jnp.mean(grouped, axis=(1, 2, 4), keepdims=True)
    centered = grouped - grp_mean
    grp_var = jnp.mean(jnp.square(centered), axis=(1, 2, 4), keepdims=True)
    normed = (centered * lax.rsqrt(grp_var + NORM_EPS)).reshape(out_shape)
    return jax.nn.relu(normed * affine[1] + affine[2]).astype(jnp.bfloat16)


def reference(image, down_w1, down_v1, refine_w1, refine_v1, down_w2, down_v2, refine_w2, refine_v2, down_w3, down_v3, refine_w3, refine_v3):
    stages = ((down_w1, down_v1, refine_w1, refine_v1), (down_w2, down_v2, refine_w2, refine_v2), (down_w3, down_v3, refine_w3, refine_v3))

    def one_image(single):
        current = single[None]
        for down_w, down_v, refine_w, refine_v in stages:
            current = conv_norm(current, down_w, down_v, 2)
            current = conv_norm(current, refine_w, refine_v, 1)
        return current[0]

    return lax.map(one_image, image)
```

```python
import jax
import jax.numpy as jnp
from jax import lax
from jax.sharding import PartitionSpec as P

NORM_GROUPS = 8
NORM_EPS = 1e-5


def conv_norm(inputs, kernel, affine, stride):
    summed = lax.conv_general_dilated(inputs, kernel, (stride, stride), ((1, 1), (1, 1)), dimension_numbers=("NHWC", "HWIO", "NHWC"), preferred_element_type=jnp.float32) + affine[0]
    out_shape = summed.shape
    per_group = out_shape[3] // NORM_GROUPS
    pixel_count = out_shape[1] * out_shape[2] * per_group
    part_sums = jnp.stack([jnp.sum(summed, axis=(1, 2)), jnp.sum(jnp.square(summed), axis=(1, 2))])
    totals = jnp.sum(part_sums.reshape(2, out_shape[0], NORM_GROUPS, per_group), axis=3)
    grp_mean = totals[0] / pixel_count
    grp_var = jnp.maximum(totals[1] / pixel_count - jnp.square(grp_mean), 0.0)
    inv_std = lax.rsqrt(grp_var + NORM_EPS)
    chan_scale = jnp.repeat(inv_std, per_group, axis=1) * affine[1]
    chan_shift = affine[2] - jnp.repeat(grp_mean * inv_std, per_group, axis=1) * affine[1]
    return jax.nn.relu(summed * chan_scale[:, None, None, :] + chan_shift[:, None, None, :]).astype(jnp.bfloat16)


def solution(mesh):
    rows = mesh.shape["h"]
    cols = mesh.shape["w"]
    act_spec = P("batch", "h", "w")

    def local_forward(tile, *params):
        count, height, width, _ = tile.shape
        share = count // (rows * cols)
        sent = tile.reshape(rows * cols, share, height, width)
        got = lax.all_to_all(sent, ("h", "w"), 0, 0, tiled=True)
        got = got.reshape(rows, cols, share, height, width)
        current = got.transpose(2, 0, 3, 1, 4).reshape(share, rows * height, cols * width, 1)
        for stage in range(3):
            down_w, down_v, refine_w, refine_v = params[4 * stage:4 * stage + 4]
            current = conv_norm(current, down_w, down_v, 2)
            current = conv_norm(current, refine_w, refine_v, 1)
        chan = current.shape[3]
        out_h = current.shape[1] // rows
        out_w = current.shape[2] // cols
        back = current.reshape(share, rows, out_h, cols, out_w, chan).transpose(1, 3, 0, 2, 4, 5)
        back = back.reshape(rows * cols, share, out_h, out_w, chan)
        back = lax.all_to_all(back, ("h", "w"), 0, 0, tiled=True)
        return back.reshape(count, out_h, out_w, chan)

    return jax.shard_map(local_forward, mesh=mesh, in_specs=(act_spec,) + (P(),) * 12, out_specs=act_spec, check_vma=False)
```

```python
import jax
import jax.numpy as jnp
from jax import lax
from jax.experimental import pallas as pl
from jax.experimental.pallas import tpu as pltpu
from jax.sharding import PartitionSpec as P

NORM_EPS = 1e-5
LANE = 128
BLOCK = 256
WIDE = 1024
BF = jnp.bfloat16
F32 = jnp.float32
MESH = pl.DeviceIdType.MESH
ROWS = (8, 8, 4, 4, 2, 2)
CHANS = (64, 64, 128, 128, 256, 256)


def iota(shape, axis):
    return lax.broadcasted_iota(jnp.int32, shape, axis)


def make_kernel(share):
    chunks = share // 4

    def kernel(x_ref, w1d, v1d, w1r, v1r, w2d, v2d, w2r, v2r, w3d, v3d, w3r, v3r, o_ref,
               slab, recv, ze, zo, t1, tr1, td2, tr2, aff, gmat, smat, pmat,
               acc, zd1, zr1, zd2, zr2, zd3, fst, outb,
               send_in, recv_in, send_out, recv_out, local_out):
        wi = lax.axis_index("w")
        hi = lax.axis_index("h")
        me = hi * 4 + wi
        barrier = pltpu.get_barrier_semaphore()

        def peer(k):
            d = lax.rem(me + k, 16)
            return d, {"h": d // 4, "w": lax.rem(d, 4)}

        for k in range(1, 16):
            pl.semaphore_signal(barrier, inc=1, device_id=peer(k)[1], device_id_type=MESH)

        r, c = iota((BLOCK, BLOCK), 0), iota((BLOCK, BLOCK), 1)
        half, parity, quarter, strip = r // LANE, (r // 64) % 2, (r // 16) % 4, r % 16
        pmat[...] = (c == strip * 16 + half * 8 + quarter * 2 + parity).astype(F32).astype(BF)

        def pack(k, carry):
            d, _ = peer(k)
            rows = x_ref[pl.ds(pl.multiple_of(d * (8 * share), 32), 8 * share), :]
            turned = lax.dot_general(pmat[...], rows, (((1,), (1,)), ((), ())), preferred_element_type=F32).astype(BF)
            for ch in range(chunks):
                for q in range(4):
                    slab[ch, k, :, 32 * q:32 * q + 32] = turned[64 * q:64 * q + 64, 32 * ch:32 * ch + 32]
            return carry

        lax.fori_loop(0, 16, pack, 0)
        pl.semaphore_wait(barrier, 15)

        def in_copy(ch, k):
            _, dev = peer(k)
            return pltpu.make_async_remote_copy(
                src_ref=slab.at[ch, k], dst_ref=recv.at[ch, me], send_sem=send_in, recv_sem=recv_in.at[ch],
                device_id=dev, device_id_type=MESH)

        for ch in range(chunks):
            def send(k, carry, ch=ch):
                in_copy(ch, k).start()
                return carry
            lax.fori_loop(1, 16, send, 0)
            recv[ch, me] = slab[ch, 0]

        r, c = iota((512, 512), 0), iota((512, 512), 1)
        smat[...] = ((r // LANE == (c // 8) % 4) & ((r // 32) % 4 == c // LANE) & ((r // 8) % 4 == (c // 32) % 4)
                     & (r % 8 == c % 8)).astype(F32).astype(BF)
        r, c = iota((384, LANE), 0) % LANE, iota((384, LANE), 1)
        for s, chan in enumerate((64, LANE, BLOCK)):
            size = chan // 8
            gmat[s] = ((r % chan) // size == (c % chan) // size).astype(F32).astype(BF)
        for s, v in enumerate((v1d, v1r, v2d, v2r, v3d, v3r)):
            chan = CHANS[s]
            if chan == 64:
                aff[s, 0:3, :] = jnp.concatenate([v[...], v[...]], axis=1)
            else:
                aff[s, 0:3, :] = v[:, 0:LANE]
                if chan == BLOCK:
                    aff[s, 3:6, :] = v[:, LANE:BLOCK]
        t1[...] = jnp.zeros_like(t1)
        row, col = iota((32, WIDE), 0), iota((32, WIDE), 1) // 64
        for dh in range(3):
            base = jnp.zeros((32, WIDE), F32)
            for dw in range(3):
                tap = w1d[dh, dw:dw + 1, :].astype(F32)
                tap = jnp.concatenate([tap, tap], axis=1)
                tap = jnp.concatenate([tap] * 8, axis=1)
                base = jnp.where(row == 2 * col + dw - 1, jnp.broadcast_to(tap, (32, WIDE)), base)
            for i in range(4):
                t1[i, dh * LANE + 32 * i:dh * LANE + 32 * i + 32, :] = base.astype(BF)
        tr1[...] = jnp.zeros_like(tr1)
        td2[...] = jnp.zeros_like(td2)
        tr2[...] = jnp.zeros_like(tr2)
        for dh in range(3):
            for dw in range(3):
                tap = w1r[dh, 64 * dw:64 * dw + 64, :]
                for jo in range(4):
                    ji = jo + 1 + dw
                    tr1[dh, 64 * ji:64 * ji + 64, 64 * jo:64 * jo + 64] = tap
                tap = w2d[dh, 64 * dw:64 * dw + 64, :]
                for jo in range(2):
                    ji = 2 * jo + 1 + dw
                    td2[dh, 64 * ji:64 * ji + 64, LANE * jo:LANE * jo + LANE] = tap
                tap = w2r[dh, LANE * dw:LANE * dw + LANE, :]
                for jo in range(2):
                    ji = jo + dw
                    tr2[dh, LANE * ji:LANE * ji + LANE, LANE * jo:LANE * jo + LANE] = tap

        top = iota((64, BLOCK), 0) == 0
        bottom = iota((64, BLOCK), 0) == 63

        def taps(ref, j, rows, stride, lo, hi_):
            pieces = []
            for dh in range(3):
                if stride == 1:
                    piece = ref[j, :, dh:dh + rows, :, lo:hi_]
                    pieces.append(piece.reshape(64 * rows, hi_ - lo))
                else:
                    pieces.append(jnp.concatenate(
                        [ref[j, h, 2 * l + dh, :, lo:hi_] for h in range(4) for l in range(rows)], axis=0))
            return jnp.concatenate(pieces, axis=1)

        def conv(j, s, b, i):
            rows = ROWS[s]
            m = 64 * rows
            lo = BLOCK * b
            if s == 0:
                lhs = jnp.concatenate([zo[:, 0:8].reshape(m, LANE), ze[...].reshape(m, LANE),
                                       zo[:, 1:9].reshape(m, LANE)], axis=1)
                rhs = t1[i, :, lo:lo + BLOCK]
            elif s in (1, 3):
                ref, mat = ((zd1, tr1), (zd2, tr2))[s // 2]
                first, last = (LANE if b == 0 else 0), (384 if b == 3 else 512)
                lhs = taps(ref, j, rows, 1, lo - LANE + first, lo - LANE + last)
                rhs = mat[:, first:last, :].reshape(3 * (last - first), BLOCK)
            elif s in (2, 4):
                ref, mat = ((zr1, td2), (zr2, w3d))[s // 2 - 1]
                first = LANE if b == 0 else 0
                lhs = taps(ref, j, rows, 2, lo - LANE + first, lo + BLOCK)
                rhs = mat[:, first:384, :].reshape(3 * (384 - first), BLOCK)
            else:
                first, last = (BLOCK if b == 0 else 0), (512 if b == 3 else 768)
                lhs = taps(zd3, j, rows, 1, lo - BLOCK + first, lo - BLOCK + last)
                rhs = w3r[:, first:last, :].reshape(3 * (last - first), BLOCK)
            out = jnp.dot(lhs, rhs, preferred_element_type=F32)
            acc[j, 0:m, lo:lo + BLOCK] = out
            tall = out.reshape(m // 8, 8, BLOCK)
            return jnp.sum(tall, axis=0), jnp.sum(tall * tall, axis=0)

        def finish(s, parts):
            m, chan = 64 * ROWS[s], CHANS[s]
            sums = parts[0][0] + parts[1][0] + parts[2][0] + parts[3][0]
            sqs = parts[0][1] + parts[1][1] + parts[2][1] + parts[3][1]
            if chan == BLOCK:
                sides, per_lane = [(sums[:, 0:LANE], sqs[:, 0:LANE]), (sums[:, LANE:], sqs[:, LANE:])], 4.0 * m
            else:
                sides, per_lane = [(sums[:, 0:LANE] + sums[:, LANE:], sqs[:, 0:LANE] + sqs[:, LANE:])], 8.0 * m
            count = float(m * WIDE // 8)
            row16 = iota((16, LANE), 0)
            packed = jnp.zeros((16, LANE), F32)
            for n, (one, two) in enumerate(sides):
                bias = aff[s, 3 * n:3 * n + 1, :]
                one = jnp.sum(one, axis=0, keepdims=True)
                two = jnp.sum(two, axis=0, keepdims=True)
                total = one + per_lane * bias
                square = two + bias * (one + total)
                packed = jnp.where(row16 == 2 * n, total, jnp.where(row16 == 2 * n + 1, square, packed))
            high = packed.astype(BF)
            rest = packed - high.astype(F32)
            mid = rest.astype(BF)
            low = (rest - mid.astype(F32)).astype(BF)
            totals = jnp.dot(jnp.concatenate([high, mid, low], axis=1), gmat[s // 2], preferred_element_type=F32)
            scales, shifts = [], []
            for n in range(len(sides)):
                bias, gain, beta = (aff[s, 3 * n + t:3 * n + t + 1, :] for t in range(3))
                mean = totals[2 * n:2 * n + 1] * (1.0 / count)
                var = jnp.maximum(totals[2 * n + 1:2 * n + 2] * (1.0 / count) - mean * mean, 0.0)
                scale = lax.rsqrt(var + NORM_EPS) * gain
                scales.append(scale)
                shifts.append(beta + (bias - mean) * scale)
            if len(sides) == 1:
                scales, shifts = scales * 2, shifts * 2
            return jnp.concatenate(scales, axis=1), jnp.concatenate(shifts, axis=1)

        def norm(j, s, b, affine):
            rows = ROWS[s]
            m = 64 * rows
            lo = BLOCK * b
            z = jnp.maximum(acc[j, 0:m, lo:lo + BLOCK] * affine[0] + affine[1], 0.0).reshape(4, rows, 16, BLOCK)
            if s == 5:
                for h in range(4):
                    for l in range(2):
                        for t in range(2):
                            fst[j, 2 * (4 * h + b) + t, pl.ds(l, 16, stride=2), :] = z[h, l, :, LANE * t:LANE * t + LANE]
                return
            ref = (zd1, zr1, zd2, zr2, zd3)[s]
            ref[j, :, 1:1 + rows, :, lo:lo + BLOCK] = z.astype(BF)
            edge = pltpu.roll(z[:, rows - 1].reshape(64, BLOCK), 1, axis=0)
            ref[j, :, 0, :, lo:lo + BLOCK] = jnp.where(top, 0.0, edge).reshape(4, 16, BLOCK).astype(BF)
            if s in (0, 2, 4):
                edge = pltpu.roll(z[:, 0].reshape(64, BLOCK), 63, axis=0)
                ref[j, :, 1 + rows, :, lo:lo + BLOCK] = jnp.where(bottom, 0.0, edge).reshape(4, 16, BLOCK).astype(BF)

        def out_copy(n, k):
            d, dev = peer(k)
            return pltpu.make_async_remote_copy(
                src_ref=outb.at[n, d], dst_ref=o_ref.at[me * share + n], send_sem=send_out, recv_sem=recv_out,
                device_id=dev, device_id_type=MESH)

        def own_copy(n):
            return pltpu.make_async_copy(outb.at[n, me], o_ref.at[me * share + n], local_out)

        def emit(j, n):
            for d in range(16):
                outb[n, d] = jnp.concatenate([fst[j, 2 * d], fst[j, 2 * d + 1]], axis=1).astype(BF)
            own_copy(n).start()
            for k in range(1, 16):
                out_copy(n, k).start()

        def pair_body(p, carry):
            pair_head(p)
            return carry

        def pair_head(p):
            ch = p // 2

            @pl.when(lax.rem(p, 2) == 0)
            def _():
                pltpu.make_async_copy(recv.at[ch, 0:15], recv.at[ch, 0:15], recv_in.at[ch]).wait()
                wide = jnp.concatenate([
                    jnp.concatenate([recv[ch, 4 * h + w] for h in range(4)], axis=0) for w in range(4)], axis=1)
                spread = jnp.dot(wide, smat[...], preferred_element_type=F32)
                for half in range(2):
                    even = spread[:, BLOCK * half:BLOCK * half + LANE].astype(BF).reshape(4, 4, 16, LANE)
                    odd = spread[:, BLOCK * half + LANE:BLOCK * half + BLOCK].reshape(4, 4, 16, LANE)
                    ze[:, 4 * half:4 * half + 4] = even
                    zo[:, 1 + 4 * half:5 + 4 * half] = odd.astype(BF)
                    if half == 1:
                        edge = pltpu.roll(odd[:, 3].reshape(64, LANE), 1, axis=0)
                        edge = jnp.where(iota((64, LANE), 0) == 0, 0.0, edge)
                        zo[:, 0] = edge.astype(BF).reshape(4, 16, LANE)

            base = 2 * lax.rem(p, 2)
            waiting = None
            for s in range(6):
                for j in range(2):
                    parts = []
                    for b in range(4):
                        parts.append(conv(j, s, b, base + j))
                        if waiting is not None:
                            norm(*waiting[0:2], b, waiting[2])
                    waiting = (j, s, finish(s, parts))
                    if s == 5 and j == 1:
                        emit(0, 2 * p)
            for b in range(4):
                norm(*waiting[0:2], b, waiting[2])
            emit(1, 2 * p + 1)

        lax.fori_loop(0, share // 2, pair_body, 0)

        pltpu.make_async_copy(slab.at[:, 0:15], slab.at[:, 0:15], send_in).wait()
        pltpu.make_async_copy(outb.at[:, 0:15], outb.at[:, 0:15], send_out).wait()
        pltpu.make_async_copy(o_ref.at[0:15 * share], o_ref.at[0:15 * share], recv_out).wait()
        pltpu.make_async_copy(o_ref.at[0:share], o_ref.at[0:share], local_out).wait()

    return kernel


def encode(tile, params):
    count = tile.shape[0]
    share = count // 16
    chunks = share // 4
    rows = tile.reshape(count, BLOCK, 8).transpose(0, 2, 1).reshape(count * 8, BLOCK)
    weights = []
    for n, param in enumerate(params):
        if n == 0:
            weights.append(param.reshape(3, 3, 64))
        elif n % 2 == 0:
            weights.append(param.reshape(3, 3 * param.shape[2], param.shape[3]))
        else:
            weights.append(param)
    vmem = pl.BlockSpec(memory_space=pltpu.VMEM)
    return pl.pallas_call(
        make_kernel(share),
        out_shape=jax.ShapeDtypeStruct((count, 32, BLOCK), BF),
        in_specs=[vmem] * 13,
        out_specs=pl.BlockSpec(memory_space=pl.ANY),
        scratch_shapes=[
            pltpu.VMEM((chunks, 16, 64, LANE), BF),
            pltpu.VMEM((chunks, 16, 64, LANE), BF),
            pltpu.VMEM((4, 8, 16, LANE), BF),
            pltpu.VMEM((4, 9, 16, LANE), BF),
            pltpu.VMEM((4, 384, WIDE), BF),
            pltpu.VMEM((3, 512, BLOCK), BF),
            pltpu.VMEM((3, 384, BLOCK), BF),
            pltpu.VMEM((3, 512, BLOCK), BF),
            pltpu.VMEM((6, 8, LANE), F32),
            pltpu.VMEM((3, 384, LANE), BF),
            pltpu.VMEM((512, 512), BF),
            pltpu.VMEM((BLOCK, BLOCK), BF),
            pltpu.VMEM((2, 512, WIDE), F32),
            pltpu.VMEM((2, 4, 10, 16, WIDE), BF),
            pltpu.VMEM((2, 4, 9, 16, WIDE), BF),
            pltpu.VMEM((2, 4, 6, 16, WIDE), BF),
            pltpu.VMEM((2, 4, 5, 16, WIDE), BF),
            pltpu.VMEM((2, 4, 4, 16, WIDE), BF),
            pltpu.VMEM((2, 32, 32, LANE), F32),
            pltpu.VMEM((share, 16, 32, BLOCK), BF),
            pltpu.SemaphoreType.DMA,
            pltpu.SemaphoreType.DMA((chunks,)),
            pltpu.SemaphoreType.DMA,
            pltpu.SemaphoreType.DMA,
            pltpu.SemaphoreType.DMA,
        ],
        compiler_params=pltpu.CompilerParams(
            collective_id=0, has_side_effects=True, vmem_limit_bytes=60 * WIDE * WIDE),
        name="encoder",
    )(rows, *weights)


def solution(mesh):
    act_spec = P("batch", "h", "w")

    def local_forward(tile, *params):
        return encode(tile, params)[:, :, None, :]

    return jax.shard_map(local_forward, mesh=mesh, in_specs=(act_spec,) + (P(),) * 12, out_specs=act_spec, check_vma=False)
```

```python
import jax
import jax.numpy as jnp
from jax import lax
from jax.experimental import pallas as pl
from jax.experimental.pallas import tpu as pltpu
from jax.sharding import PartitionSpec as P

NORM_EPS = 1e-5
LANE = 128
BLOCK = 256
WIDE = 1024
CHUNK = 512
BF = jnp.bfloat16
F32 = jnp.float32
MESH = pl.DeviceIdType.MESH
ROWS = (8, 8, 4, 4, 2, 2)
CHANS = (64, 64, 128, 128, 256, 256)


def iota(shape, axis):
    return lax.broadcasted_iota(jnp.int32, shape, axis)


def make_kernel(share):
    chunks = share // 4

    def kernel(x_ref, w1d, v1d, w1r, v1r, w2d, v2d, w2r, v2r, w3d, v3d, w3r, v3r, o_ref,
               slab, recv, ze, zo, t1, tr1, td2, tr2, aff, gmat, smat, pmat,
               acc, zd1, zr1, zd2, zr2, zd3, fst, outb,
               send_in, recv_in, send_out, recv_out, local_out):
        wi = lax.axis_index("w")
        hi = lax.axis_index("h")
        me = hi * 4 + wi
        barrier = pltpu.get_barrier_semaphore()

        def peer(k):
            d = lax.rem(me + k, 16)
            return d, {"h": d // 4, "w": lax.rem(d, 4)}

        for k in range(1, 16):
            pl.semaphore_signal(barrier, inc=1, device_id=peer(k)[1], device_id_type=MESH)

        r, c = iota((BLOCK, BLOCK), 0), iota((BLOCK, BLOCK), 1)
        half, parity, quarter, strip = r // LANE, (r // 64) % 2, (r // 16) % 4, r % 16
        pmat[...] = (c == strip * 16 + half * 8 + quarter * 2 + parity).astype(F32).astype(BF)

        def pack(k, carry):
            d, _ = peer(k)
            rows = x_ref[pl.ds(pl.multiple_of(d * (8 * share), 32), 8 * share), :]
            turned = lax.dot_general(pmat[...], rows, (((1,), (1,)), ((), ())), preferred_element_type=F32).astype(BF)
            for ch in range(chunks):
                for q in range(4):
                    slab[ch, k, :, 32 * q:32 * q + 32] = turned[64 * q:64 * q + 64, 32 * ch:32 * ch + 32]
            return carry

        lax.fori_loop(0, 16, pack, 0)
        pl.semaphore_wait(barrier, 15)

        def in_copy(ch, k):
            _, dev = peer(k)
            return pltpu.make_async_remote_copy(
                src_ref=slab.at[ch, k], dst_ref=recv.at[ch, me], send_sem=send_in, recv_sem=recv_in.at[ch],
                device_id=dev, device_id_type=MESH)

        for ch in range(chunks):
            def send(k, carry, ch=ch):
                in_copy(ch, k).start()
                return carry
            lax.fori_loop(1, 16, send, 0)
            recv[ch, me] = slab[ch, 0]

        r, c = iota((512, 512), 0), iota((512, 512), 1)
        smat[...] = ((r // LANE == (c // 8) % 4) & ((r // 32) % 4 == c // LANE) & ((r // 8) % 4 == (c // 32) % 4)
                     & (r % 8 == c % 8)).astype(F32).astype(BF)
        r, c = iota((384, LANE), 0) % LANE, iota((384, LANE), 1)
        for s, chan in enumerate((64, LANE, BLOCK)):
            size = chan // 8
            gmat[s] = ((r % chan) // size == (c % chan) // size).astype(F32).astype(BF)
        for s, v in enumerate((v1d, v1r, v2d, v2r, v3d, v3r)):
            chan = CHANS[s]
            if chan == 64:
                aff[s, 0:3, :] = jnp.concatenate([v[...], v[...]], axis=1)
            else:
                aff[s, 0:3, :] = v[:, 0:LANE]
                if chan == BLOCK:
                    aff[s, 3:6, :] = v[:, LANE:BLOCK]
        t1[...] = jnp.zeros_like(t1)
        row, col = iota((32, WIDE), 0), iota((32, WIDE), 1) // 64
        for dh in range(3):
            base = jnp.zeros((32, WIDE), F32)
            for dw in range(3):
                tap = w1d[dh, dw:dw + 1, :].astype(F32)
                tap = jnp.concatenate([tap, tap], axis=1)
                tap = jnp.concatenate([tap] * 8, axis=1)
                base = jnp.where(row == 2 * col + dw - 1, jnp.broadcast_to(tap, (32, WIDE)), base)
            for i in range(4):
                t1[i, dh * LANE + 32 * i:dh * LANE + 32 * i + 32, :] = base.astype(BF)
        tr1[...] = jnp.zeros_like(tr1)
        td2[...] = jnp.zeros_like(td2)
        tr2[...] = jnp.zeros_like(tr2)
        for dh in range(3):
            for dw in range(3):
                tap = w1r[dh, 64 * dw:64 * dw + 64, :]
                for jo in range(4):
                    ji = jo + 1 + dw
                    tr1[dh, 64 * ji:64 * ji + 64, 64 * jo:64 * jo + 64] = tap
                tap = w2d[dh, 64 * dw:64 * dw + 64, :]
                for jo in range(2):
                    ji = 2 * jo + 1 + dw
                    td2[dh, 64 * ji:64 * ji + 64, LANE * jo:LANE * jo + LANE] = tap
                tap = w2r[dh, LANE * dw:LANE * dw + LANE, :]
                for jo in range(2):
                    ji = jo + dw
                    tr2[dh, LANE * ji:LANE * ji + LANE, LANE * jo:LANE * jo + LANE] = tap

        top = iota((64, BLOCK), 0) == 0
        bottom = iota((64, BLOCK), 0) == 63

        def taps(ref, j, rows, stride, lo, hi_, h0, h1):
            pieces = []
            for dh in range(3):
                if stride == 1:
                    piece = ref[j, h0:h1, dh:dh + rows, :, lo:hi_]
                    pieces.append(piece.reshape((h1 - h0) * 16 * rows, hi_ - lo))
                else:
                    pieces.append(jnp.concatenate(
                        [ref[j, h, 2 * l + dh, :, lo:hi_] for h in range(h0, h1) for l in range(rows)], axis=0))
            return jnp.concatenate(pieces, axis=1)

        def conv(j, s, b, i):
            rows = ROWS[s]
            lo = BLOCK * b
            step = min(4, CHUNK // (16 * rows))
            sums = sqs = None
            for h0 in range(0, 4, step):
                h1 = h0 + step
                m = 16 * rows * step
                if s == 0:
                    lhs = jnp.concatenate([zo[h0:h1, 0:8].reshape(m, LANE), ze[h0:h1].reshape(m, LANE),
                                           zo[h0:h1, 1:9].reshape(m, LANE)], axis=1)
                    rhs = t1[i, :, lo:lo + BLOCK]
                elif s in (1, 3):
                    ref, mat = ((zd1, tr1), (zd2, tr2))[s // 2]
                    first, last = (LANE if b == 0 else 0), (384 if b == 3 else 512)
                    lhs = taps(ref, j, rows, 1, lo - LANE + first, lo - LANE + last, h0, h1)
                    rhs = mat[:, first:last, :].reshape(3 * (last - first), BLOCK)
                elif s in (2, 4):
                    ref, mat = ((zr1, td2), (zr2, w3d))[s // 2 - 1]
                    first = LANE if b == 0 else 0
                    lhs = taps(ref, j, rows, 2, lo - LANE + first, lo + BLOCK, h0, h1)
                    rhs = mat[:, first:384, :].reshape(3 * (384 - first), BLOCK)
                else:
                    first, last = (BLOCK if b == 0 else 0), (512 if b == 3 else 768)
                    lhs = taps(zd3, j, rows, 1, lo - BLOCK + first, lo - BLOCK + last, h0, h1)
                    rhs = w3r[:, first:last, :].reshape(3 * (last - first), BLOCK)
                out = jnp.dot(lhs, rhs, preferred_element_type=F32)
                at = 16 * rows * h0
                acc[j, at:at + m, lo:lo + BLOCK] = out
                tall = out.reshape(m // 8, 8, BLOCK)
                one, two = jnp.sum(tall, axis=0), jnp.sum(tall * tall, axis=0)
                sums, sqs = (one, two) if sums is None else (sums + one, sqs + two)
            return sums, sqs

        def finish(s, parts):
            m, chan = 64 * ROWS[s], CHANS[s]
            sums = parts[0][0] + parts[1][0] + parts[2][0] + parts[3][0]
            sqs = parts[0][1] + parts[1][1] + parts[2][1] + parts[3][1]
            if chan == BLOCK:
                sides, per_lane = [(sums[:, 0:LANE], sqs[:, 0:LANE]), (sums[:, LANE:], sqs[:, LANE:])], 4.0 * m
            else:
                sides, per_lane = [(sums[:, 0:LANE] + sums[:, LANE:], sqs[:, 0:LANE] + sqs[:, LANE:])], 8.0 * m
            count = float(m * WIDE // 8)
            row16 = iota((16, LANE), 0)
            packed = jnp.zeros((16, LANE), F32)
            for n, (one, two) in enumerate(sides):
                bias = aff[s, 3 * n:3 * n + 1, :]
                one = jnp.sum(one, axis=0, keepdims=True)
                two = jnp.sum(two, axis=0, keepdims=True)
                total = one + per_lane * bias
                square = two + bias * (one + total)
                packed = jnp.where(row16 == 2 * n, total, jnp.where(row16 == 2 * n + 1, square, packed))
            high = packed.astype(BF)
            rest = packed - high.astype(F32)
            mid = rest.astype(BF)
            low = (rest - mid.astype(F32)).astype(BF)
            totals = jnp.dot(jnp.concatenate([high, mid, low], axis=1), gmat[s // 2], preferred_element_type=F32)
            scales, shifts = [], []
            for n in range(len(sides)):
                bias, gain, beta = (aff[s, 3 * n + t:3 * n + t + 1, :] for t in range(3))
                mean = totals[2 * n:2 * n + 1] * (1.0 / count)
                var = jnp.maximum(totals[2 * n + 1:2 * n + 2] * (1.0 / count) - mean * mean, 0.0)
                scale = lax.rsqrt(var + NORM_EPS) * gain
                scales.append(scale)
                shifts.append(beta + (bias - mean) * scale)
            if len(sides) == 1:
                scales, shifts = scales * 2, shifts * 2
            return jnp.concatenate(scales, axis=1), jnp.concatenate(shifts, axis=1)

        def norm(j, s, b, affine):
            rows = ROWS[s]
            m = 64 * rows
            lo = BLOCK * b
            z = jnp.maximum(acc[j, 0:m, lo:lo + BLOCK] * affine[0] + affine[1], 0.0).reshape(4, rows, 16, BLOCK)
            if s == 5:
                for h in range(4):
                    for l in range(2):
                        for t in range(2):
                            fst[j, 2 * (4 * h + b) + t, pl.ds(l, 16, stride=2), :] = z[h, l, :, LANE * t:LANE * t + LANE]
                return
            ref = (zd1, zr1, zd2, zr2, zd3)[s]
            ref[j, :, 1:1 + rows, :, lo:lo + BLOCK] = z.astype(BF)
            edge = pltpu.roll(z[:, rows - 1].reshape(64, BLOCK), 1, axis=0)
            ref[j, :, 0, :, lo:lo + BLOCK] = jnp.where(top, 0.0, edge).reshape(4, 16, BLOCK).astype(BF)
            if s in (0, 2, 4):
                edge = pltpu.roll(z[:, 0].reshape(64, BLOCK), 63, axis=0)
                ref[j, :, 1 + rows, :, lo:lo + BLOCK] = jnp.where(bottom, 0.0, edge).reshape(4, 16, BLOCK).astype(BF)

        def out_copy(n, k):
            d, dev = peer(k)
            return pltpu.make_async_remote_copy(
                src_ref=outb.at[n, d], dst_ref=o_ref.at[me * share + n], send_sem=send_out, recv_sem=recv_out,
                device_id=dev, device_id_type=MESH)

        def own_copy(n):
            return pltpu.make_async_copy(outb.at[n, me], o_ref.at[me * share + n], local_out)

        def emit(j, n):
            for d in range(16):
                outb[n, d] = jnp.concatenate([fst[j, 2 * d], fst[j, 2 * d + 1]], axis=1).astype(BF)
            own_copy(n).start()
            for k in range(1, 16):
                out_copy(n, k).start()

        def pair_body(p, carry):
            pair_head(p)
            return carry

        def pair_head(p):
            ch = p // 2

            @pl.when(lax.rem(p, 2) == 0)
            def _():
                pltpu.make_async_copy(recv.at[ch, 0:15], recv.at[ch, 0:15], recv_in.at[ch]).wait()
                wide = jnp.concatenate([
                    jnp.concatenate([recv[ch, 4 * h + w] for h in range(4)], axis=0) for w in range(4)], axis=1)
                spread = jnp.dot(wide, smat[...], preferred_element_type=F32)
                for half in range(2):
                    even = spread[:, BLOCK * half:BLOCK * half + LANE].astype(BF).reshape(4, 4, 16, LANE)
                    odd = spread[:, BLOCK * half + LANE:BLOCK * half + BLOCK].reshape(4, 4, 16, LANE)
                    ze[:, 4 * half:4 * half + 4] = even
                    zo[:, 1 + 4 * half:5 + 4 * half] = odd.astype(BF)
                    if half == 1:
                        edge = pltpu.roll(odd[:, 3].reshape(64, LANE), 1, axis=0)
                        edge = jnp.where(iota((64, LANE), 0) == 0, 0.0, edge)
                        zo[:, 0] = edge.astype(BF).reshape(4, 16, LANE)

            base = 2 * lax.rem(p, 2)
            waiting = None
            for s in range(6):
                for j in range(2):
                    parts = []
                    for b in range(4):
                        parts.append(conv(j, s, b, base + j))
                        if waiting is not None:
                            norm(*waiting[0:2], b, waiting[2])
                    waiting = (j, s, finish(s, parts))
                    if s == 5 and j == 1:
                        emit(0, 2 * p)
            for b in range(4):
                norm(*waiting[0:2], b, waiting[2])
            emit(1, 2 * p + 1)

        lax.fori_loop(0, share // 2, pair_body, 0)

        pltpu.make_async_copy(slab.at[:, 0:15], slab.at[:, 0:15], send_in).wait()
        pltpu.make_async_copy(outb.at[:, 0:15], outb.at[:, 0:15], send_out).wait()
        pltpu.make_async_copy(o_ref.at[0:15 * share], o_ref.at[0:15 * share], recv_out).wait()
        pltpu.make_async_copy(o_ref.at[0:share], o_ref.at[0:share], local_out).wait()

    return kernel


def encode(tile, params):
    count = tile.shape[0]
    share = count // 16
    chunks = share // 4
    rows = tile.reshape(count, BLOCK, 8).transpose(0, 2, 1).reshape(count * 8, BLOCK)
    weights = []
    for n, param in enumerate(params):
        if n == 0:
            weights.append(param.reshape(3, 3, 64))
        elif n % 2 == 0:
            weights.append(param.reshape(3, 3 * param.shape[2], param.shape[3]))
        else:
            weights.append(param)
    vmem = pl.BlockSpec(memory_space=pltpu.VMEM)
    return pl.pallas_call(
        make_kernel(share),
        out_shape=jax.ShapeDtypeStruct((count, 32, BLOCK), BF),
        in_specs=[vmem] * 13,
        out_specs=pl.BlockSpec(memory_space=pl.ANY),
        scratch_shapes=[
            pltpu.VMEM((chunks, 16, 64, LANE), BF),
            pltpu.VMEM((chunks, 16, 64, LANE), BF),
            pltpu.VMEM((4, 8, 16, LANE), BF),
            pltpu.VMEM((4, 9, 16, LANE), BF),
            pltpu.VMEM((4, 384, WIDE), BF),
            pltpu.VMEM((3, 512, BLOCK), BF),
            pltpu.VMEM((3, 384, BLOCK), BF),
            pltpu.VMEM((3, 512, BLOCK), BF),
            pltpu.VMEM((6, 8, LANE), F32),
            pltpu.VMEM((3, 384, LANE), BF),
            pltpu.VMEM((512, 512), BF),
            pltpu.VMEM((BLOCK, BLOCK), BF),
            pltpu.VMEM((2, 512, WIDE), F32),
            pltpu.VMEM((2, 4, 10, 16, WIDE), BF),
            pltpu.VMEM((2, 4, 9, 16, WIDE), BF),
            pltpu.VMEM((2, 4, 6, 16, WIDE), BF),
            pltpu.VMEM((2, 4, 5, 16, WIDE), BF),
            pltpu.VMEM((2, 4, 4, 16, WIDE), BF),
            pltpu.VMEM((2, 32, 32, LANE), F32),
            pltpu.VMEM((share, 16, 32, BLOCK), BF),
            pltpu.SemaphoreType.DMA,
            pltpu.SemaphoreType.DMA((chunks,)),
            pltpu.SemaphoreType.DMA,
            pltpu.SemaphoreType.DMA,
            pltpu.SemaphoreType.DMA,
        ],
        compiler_params=pltpu.CompilerParams(
            collective_id=0, has_side_effects=True, vmem_limit_bytes=30 * WIDE * WIDE),
        name="encoder",
    )(rows, *weights)


def solution(mesh):
    act_spec = P("batch", "h", "w")

    def local_forward(tile, *params):
        return encode(tile, params)[:, :, None, :]

    return jax.shard_map(local_forward, mesh=mesh, in_specs=(act_spec,) + (P(),) * 12, out_specs=act_spec, check_vma=False)
```

```python
import jax
import jax.numpy as jnp
from jax import lax
from jax.experimental import pallas as pl
from jax.experimental.pallas import tpu as pltpu
from jax.sharding import PartitionSpec as P

NORM_EPS = 1e-5
LANE = 128
BLOCK = 256
WIDE = 1024
CHUNK = 512
ARGS = 13
BF = jnp.bfloat16
F32 = jnp.float32
MESH = pl.DeviceIdType.MESH
ROWS = (8, 8, 4, 4, 2, 2)
CHANS = (64, 64, 128, 128, 256, 256)


def iota(shape, axis):
    return lax.broadcasted_iota(jnp.int32, shape, axis)


def make_kernel(share):
    chunks = share // 4

    def kernel(*refs):
        inputs, (o_ref, *refs) = refs[:ARGS], refs[ARGS:]
        local, refs = refs[:ARGS], refs[ARGS:]
        body(inputs, local, o_ref, *refs)

    def body(inputs, local, o_ref, load_sem,
               slab, recv, ze, zo, t1, tr1, td2, tr2, aff, gmat, smat, pmat,
               acc, zd1, zr1, zd2, zr2, zd3, fst, outb,
               send_in, recv_in, send_out, recv_out, local_out):
        x_ref, w1d, v1d, w1r, v1r, w2d, v2d, w2r, v2r, w3d, v3d, w3r, v3r = local
        loads = [pltpu.make_async_copy(inputs[n], local[n], load_sem.at[n]) for n in range(ARGS)]
        for load in loads:
            load.start()
        wi = lax.axis_index("w")
        hi = lax.axis_index("h")
        me = hi * 4 + wi
        barrier = pltpu.get_barrier_semaphore()

        def peer(k):
            d = lax.rem(me + k, 16)
            return d, {"h": d // 4, "w": lax.rem(d, 4)}

        for k in range(1, 16):
            pl.semaphore_signal(barrier, inc=1, device_id=peer(k)[1], device_id_type=MESH)

        r, c = iota((BLOCK, BLOCK), 0), iota((BLOCK, BLOCK), 1)
        half, parity, quarter, strip = r // LANE, (r // 64) % 2, (r // 16) % 4, r % 16
        pmat[...] = (c == strip * 16 + half * 8 + quarter * 2 + parity).astype(F32).astype(BF)

        def pack(k, carry):
            d, _ = peer(k)
            rows = x_ref[pl.ds(pl.multiple_of(d * (8 * share), 32), 8 * share), :]
            turned = lax.dot_general(pmat[...], rows, (((1,), (1,)), ((), ())), preferred_element_type=F32).astype(BF)
            for ch in range(chunks):
                for q in range(4):
                    slab[ch, k, :, 32 * q:32 * q + 32] = turned[64 * q:64 * q + 64, 32 * ch:32 * ch + 32]
            return carry

        loads[0].wait()
        lax.fori_loop(0, 16, pack, 0)
        pl.semaphore_wait(barrier, 15)

        def in_copy(ch, k):
            _, dev = peer(k)
            return pltpu.make_async_remote_copy(
                src_ref=slab.at[ch, k], dst_ref=recv.at[ch, me], send_sem=send_in, recv_sem=recv_in.at[ch],
                device_id=dev, device_id_type=MESH)

        for ch in range(chunks):
            def send(k, carry, ch=ch):
                in_copy(ch, k).start()
                return carry
            lax.fori_loop(1, 16, send, 0)
            recv[ch, me] = slab[ch, 0]

        for load in loads[1:]:
            load.wait()
        r, c = iota((512, 512), 0), iota((512, 512), 1)
        smat[...] = ((r // LANE == (c // 8) % 4) & ((r // 32) % 4 == c // LANE) & ((r // 8) % 4 == (c // 32) % 4)
                     & (r % 8 == c % 8)).astype(F32).astype(BF)
        r, c = iota((384, LANE), 0) % LANE, iota((384, LANE), 1)
        for s, chan in enumerate((64, LANE, BLOCK)):
            size = chan // 8
            gmat[s] = ((r % chan) // size == (c % chan) // size).astype(F32).astype(BF)
        for s, v in enumerate((v1d, v1r, v2d, v2r, v3d, v3r)):
            chan = CHANS[s]
            if chan == 64:
                aff[s, 0:3, :] = jnp.concatenate([v[...], v[...]], axis=1)
            else:
                aff[s, 0:3, :] = v[:, 0:LANE]
                if chan == BLOCK:
                    aff[s, 3:6, :] = v[:, LANE:BLOCK]
        t1[...] = jnp.zeros_like(t1)
        row, col = iota((32, WIDE), 0), iota((32, WIDE), 1) // 64
        for dh in range(3):
            base = jnp.zeros((32, WIDE), F32)
            for dw in range(3):
                tap = w1d[dh, dw:dw + 1, :].astype(F32)
                tap = jnp.concatenate([tap, tap], axis=1)
                tap = jnp.concatenate([tap] * 8, axis=1)
                base = jnp.where(row == 2 * col + dw - 1, jnp.broadcast_to(tap, (32, WIDE)), base)
            for i in range(4):
                t1[i, dh * LANE + 32 * i:dh * LANE + 32 * i + 32, :] = base.astype(BF)
        tr1[...] = jnp.zeros_like(tr1)
        td2[...] = jnp.zeros_like(td2)
        tr2[...] = jnp.zeros_like(tr2)
        for dh in range(3):
            for dw in range(3):
                tap = w1r[dh, 64 * dw:64 * dw + 64, :]
                for jo in range(4):
                    ji = jo + 1 + dw
                    tr1[dh, 64 * ji:64 * ji + 64, 64 * jo:64 * jo + 64] = tap
                tap = w2d[dh, 64 * dw:64 * dw + 64, :]
                for jo in range(2):
                    ji = 2 * jo + 1 + dw
                    td2[dh, 64 * ji:64 * ji + 64, LANE * jo:LANE * jo + LANE] = tap
                tap = w2r[dh, LANE * dw:LANE * dw + LANE, :]
                for jo in range(2):
                    ji = jo + dw
                    tr2[dh, LANE * ji:LANE * ji + LANE, LANE * jo:LANE * jo + LANE] = tap

        top = iota((64, BLOCK), 0) == 0
        bottom = iota((64, BLOCK), 0) == 63

        def taps(ref, j, rows, stride, lo, hi_, h0, h1):
            pieces = []
            for dh in range(3):
                if stride == 1:
                    piece = ref[j, h0:h1, dh:dh + rows, :, lo:hi_]
                    pieces.append(piece.reshape((h1 - h0) * 16 * rows, hi_ - lo))
                else:
                    pieces.append(jnp.concatenate(
                        [ref[j, h, 2 * l + dh, :, lo:hi_] for h in range(h0, h1) for l in range(rows)], axis=0))
            return jnp.concatenate(pieces, axis=1)

        def conv(j, s, b, i):
            rows = ROWS[s]
            lo = BLOCK * b
            step = min(4, CHUNK // (16 * rows))
            sums = sqs = None
            for h0 in range(0, 4, step):
                h1 = h0 + step
                m = 16 * rows * step
                if s == 0:
                    lhs = jnp.concatenate([zo[h0:h1, 0:8].reshape(m, LANE), ze[h0:h1].reshape(m, LANE),
                                           zo[h0:h1, 1:9].reshape(m, LANE)], axis=1)
                    rhs = t1[i, :, lo:lo + BLOCK]
                elif s in (1, 3):
                    ref, mat = ((zd1, tr1), (zd2, tr2))[s // 2]
                    first, last = (LANE if b == 0 else 0), (384 if b == 3 else 512)
                    lhs = taps(ref, j, rows, 1, lo - LANE + first, lo - LANE + last, h0, h1)
                    rhs = mat[:, first:last, :].reshape(3 * (last - first), BLOCK)
                elif s in (2, 4):
                    ref, mat = ((zr1, td2), (zr2, w3d))[s // 2 - 1]
                    first = LANE if b == 0 else 0
                    lhs = taps(ref, j, rows, 2, lo - LANE + first, lo + BLOCK, h0, h1)
                    rhs = mat[:, first:384, :].reshape(3 * (384 - first), BLOCK)
                else:
                    first, last = (BLOCK if b == 0 else 0), (512 if b == 3 else 768)
                    lhs = taps(zd3, j, rows, 1, lo - BLOCK + first, lo - BLOCK + last, h0, h1)
                    rhs = w3r[:, first:last, :].reshape(3 * (last - first), BLOCK)
                out = jnp.dot(lhs, rhs, preferred_element_type=F32)
                at = 16 * rows * h0
                acc[j, at:at + m, lo:lo + BLOCK] = out
                tall = out.reshape(m // 8, 8, BLOCK)
                one, two = jnp.sum(tall, axis=0), jnp.sum(tall * tall, axis=0)
                sums, sqs = (one, two) if sums is None else (sums + one, sqs + two)
            return sums, sqs

        def finish(s, parts):
            m, chan = 64 * ROWS[s], CHANS[s]
            sums = parts[0][0] + parts[1][0] + parts[2][0] + parts[3][0]
            sqs = parts[0][1] + parts[1][1] + parts[2][1] + parts[3][1]
            if chan == BLOCK:
                sides, per_lane = [(sums[:, 0:LANE], sqs[:, 0:LANE]), (sums[:, LANE:], sqs[:, LANE:])], 4.0 * m
            else:
                sides, per_lane = [(sums[:, 0:LANE] + sums[:, LANE:], sqs[:, 0:LANE] + sqs[:, LANE:])], 8.0 * m
            count = float(m * WIDE // 8)
            row16 = iota((16, LANE), 0)
            packed = jnp.zeros((16, LANE), F32)
            for n, (one, two) in enumerate(sides):
                bias = aff[s, 3 * n:3 * n + 1, :]
                one = jnp.sum(one, axis=0, keepdims=True)
                two = jnp.sum(two, axis=0, keepdims=True)
                total = one + per_lane * bias
                square = two + bias * (one + total)
                packed = jnp.where(row16 == 2 * n, total, jnp.where(row16 == 2 * n + 1, square, packed))
            high = packed.astype(BF)
            rest = packed - high.astype(F32)
            mid = rest.astype(BF)
            low = (rest - mid.astype(F32)).astype(BF)
            totals = jnp.dot(jnp.concatenate([high, mid, low], axis=1), gmat[s // 2], preferred_element_type=F32)
            scales, shifts = [], []
            for n in range(len(sides)):
                bias, gain, beta = (aff[s, 3 * n + t:3 * n + t + 1, :] for t in range(3))
                mean = totals[2 * n:2 * n + 1] * (1.0 / count)
                var = jnp.maximum(totals[2 * n + 1:2 * n + 2] * (1.0 / count) - mean * mean, 0.0)
                scale = lax.rsqrt(var + NORM_EPS) * gain
                scales.append(scale)
                shifts.append(beta + (bias - mean) * scale)
            if len(sides) == 1:
                scales, shifts = scales * 2, shifts * 2
            return jnp.concatenate(scales, axis=1), jnp.concatenate(shifts, axis=1)

        def norm(j, s, b, affine):
            rows = ROWS[s]
            m = 64 * rows
            lo = BLOCK * b
            z = jnp.maximum(acc[j, 0:m, lo:lo + BLOCK] * affine[0] + affine[1], 0.0).reshape(4, rows, 16, BLOCK)
            if s == 5:
                for h in range(4):
                    for l in range(2):
                        for t in range(2):
                            fst[j, 2 * (4 * h + b) + t, pl.ds(l, 16, stride=2), :] = z[h, l, :, LANE * t:LANE * t + LANE]
                return
            ref = (zd1, zr1, zd2, zr2, zd3)[s]
            ref[j, :, 1:1 + rows, :, lo:lo + BLOCK] = z.astype(BF)
            edge = pltpu.roll(z[:, rows - 1].reshape(64, BLOCK), 1, axis=0)
            ref[j, :, 0, :, lo:lo + BLOCK] = jnp.where(top, 0.0, edge).reshape(4, 16, BLOCK).astype(BF)
            if s in (0, 2, 4):
                edge = pltpu.roll(z[:, 0].reshape(64, BLOCK), 63, axis=0)
                ref[j, :, 1 + rows, :, lo:lo + BLOCK] = jnp.where(bottom, 0.0, edge).reshape(4, 16, BLOCK).astype(BF)

        def out_copy(p, k):
            d, dev = peer(k)
            return pltpu.make_async_remote_copy(
                src_ref=outb.at[d, pl.ds(2 * p, 2)], dst_ref=o_ref.at[pl.ds(me * share + 2 * p, 2)],
                send_sem=send_out, recv_sem=recv_out, device_id=dev, device_id_type=MESH)

        def emit(j, n):
            for d in range(16):
                outb[d, n] = jnp.concatenate([fst[j, 2 * d], fst[j, 2 * d + 1]], axis=1).astype(BF)

        def pair_body(p, carry):
            pair_head(p)
            return carry

        def pair_head(p):
            ch = p // 2

            @pl.when(lax.rem(p, 2) == 0)
            def _():
                pltpu.make_async_copy(recv.at[ch, 0:15], recv.at[ch, 0:15], recv_in.at[ch]).wait()
                wide = jnp.concatenate([
                    jnp.concatenate([recv[ch, 4 * h + w] for h in range(4)], axis=0) for w in range(4)], axis=1)
                spread = jnp.dot(wide, smat[...], preferred_element_type=F32)
                for half in range(2):
                    even = spread[:, BLOCK * half:BLOCK * half + LANE].astype(BF).reshape(4, 4, 16, LANE)
                    odd = spread[:, BLOCK * half + LANE:BLOCK * half + BLOCK].reshape(4, 4, 16, LANE)
                    ze[:, 4 * half:4 * half + 4] = even
                    zo[:, 1 + 4 * half:5 + 4 * half] = odd.astype(BF)
                    if half == 1:
                        edge = pltpu.roll(odd[:, 3].reshape(64, LANE), 1, axis=0)
                        edge = jnp.where(iota((64, LANE), 0) == 0, 0.0, edge)
                        zo[:, 0] = edge.astype(BF).reshape(4, 16, LANE)

            base = 2 * lax.rem(p, 2)
            waiting = None
            for s in range(6):
                for j in range(2):
                    parts = []
                    for b in range(4):
                        parts.append(conv(j, s, b, base + j))
                        if waiting is not None:
                            norm(*waiting[0:2], b, waiting[2])
                    waiting = (j, s, finish(s, parts))
                    if s == 5 and j == 1:
                        @pl.when(p < share)
                        def _():
                            emit(0, 2 * p)
            for b in range(4):
                norm(*waiting[0:2], b, waiting[2])
            emit(1, 2 * p + 1)
            for k in range(1, 16):
                out_copy(p, k).start()

        lax.fori_loop(0, share // 2, pair_body, 0)

        pltpu.make_async_copy(slab.at[:, 0:15], slab.at[:, 0:15], send_in).wait()
        own = pltpu.make_async_copy(outb.at[me], o_ref.at[pl.ds(me * share, share)], local_out)
        own.start()
        own.wait()
        pltpu.make_async_copy(outb.at[0:15], outb.at[0:15], send_out).wait()
        pltpu.make_async_copy(o_ref.at[0:15 * share], o_ref.at[0:15 * share], recv_out).wait()

    return kernel


def encode(tile, params):
    count = tile.shape[0]
    share = count // 16
    chunks = share // 4
    rows = tile.reshape(count, BLOCK, 8).transpose(0, 2, 1).reshape(count * 8, BLOCK)
    weights = []
    for n, param in enumerate(params):
        if n == 0:
            weights.append(param.reshape(3, 3, 64))
        elif n % 2 == 0:
            weights.append(param.reshape(3, 3 * param.shape[2], param.shape[3]))
        else:
            weights.append(param)
    operands = [rows, *weights]
    return pl.pallas_call(
        make_kernel(share),
        out_shape=jax.ShapeDtypeStruct((count, 32, BLOCK), BF),
        in_specs=[pl.BlockSpec(memory_space=pltpu.HBM)] * ARGS,
        out_specs=pl.BlockSpec(memory_space=pl.ANY),
        scratch_shapes=[pltpu.VMEM(a.shape, a.dtype) for a in operands] + [
            pltpu.SemaphoreType.DMA((ARGS,)),
            pltpu.VMEM((chunks, 16, 64, LANE), BF),
            pltpu.VMEM((chunks, 16, 64, LANE), BF),
            pltpu.VMEM((4, 8, 16, LANE), BF),
            pltpu.VMEM((4, 9, 16, LANE), BF),
            pltpu.VMEM((4, 384, WIDE), BF),
            pltpu.VMEM((3, 512, BLOCK), BF),
            pltpu.VMEM((3, 384, BLOCK), BF),
            pltpu.VMEM((3, 512, BLOCK), BF),
            pltpu.VMEM((6, 8, LANE), F32),
            pltpu.VMEM((3, 384, LANE), BF),
            pltpu.VMEM((512, 512), BF),
            pltpu.VMEM((BLOCK, BLOCK), BF),
            pltpu.VMEM((2, 512, WIDE), F32),
            pltpu.VMEM((2, 4, 10, 16, WIDE), BF),
            pltpu.VMEM((2, 4, 9, 16, WIDE), BF),
            pltpu.VMEM((2, 4, 6, 16, WIDE), BF),
            pltpu.VMEM((2, 4, 5, 16, WIDE), BF),
            pltpu.VMEM((2, 4, 4, 16, WIDE), BF),
            pltpu.VMEM((2, 32, 32, LANE), F32),
            pltpu.VMEM((16, share, 32, BLOCK), BF),
            pltpu.SemaphoreType.DMA,
            pltpu.SemaphoreType.DMA((chunks,)),
            pltpu.SemaphoreType.DMA,
            pltpu.SemaphoreType.DMA,
            pltpu.SemaphoreType.DMA,
        ],
        compiler_params=pltpu.CompilerParams(
            collective_id=0, has_side_effects=True, vmem_limit_bytes=57 * WIDE * WIDE),
        name="encoder",
    )(*operands)


def solution(mesh):
    act_spec = P("batch", "h", "w")

    def local_forward(tile, *params):
        return encode(tile, params)[:, :, None, :]

    return jax.shard_map(local_forward, mesh=mesh, in_specs=(act_spec,) + (P(),) * 12, out_specs=act_spec, check_vma=False)
```

```python
import jax
import jax.numpy as jnp
from jax import lax
from jax.experimental import pallas as pl
from jax.experimental.pallas import tpu as pltpu
from jax.sharding import PartitionSpec as P

NORM_EPS = 1e-5
LANE = 128
BLOCK = 256
WIDE = 1024
CHUNK = 512
PAIRS = 7
SOLO = 5
ARGS = 13
BF = jnp.bfloat16
F32 = jnp.float32
MESH = pl.DeviceIdType.MESH
ROWS = (8, 8, 4, 4, 2, 2)
CHANS = (64, 64, 128, 128, 256, 256)


def iota(shape, axis):
    return lax.broadcasted_iota(jnp.int32, shape, axis)


def make_kernel(count):
    def kernel(*refs):
        inputs, (o_ref, *refs) = refs[:ARGS], refs[ARGS:]
        local, refs = refs[:ARGS], refs[ARGS:]
        body(inputs, local, o_ref, *refs)

    def body(inputs, local, o_ref, load_sem,
               slab, recv, zin, t1, tr1, td2, tr2, aff, gmat, smat, pmat, lanes,
               acc, zd1, zr1, zd2, zr2, zd3, fst, outb,
               send_in, recv_in, send_out, recv_out, local_out):
        x_ref, w1d, v1d, w1r, v1r, w2d, v2d, w2r, v2r, w3d, v3d, w3r, v3r = local
        loads = [pltpu.make_async_copy(inputs[n], local[n], load_sem.at[n]) for n in range(ARGS)]
        for load in loads:
            load.start()
        wi = lax.axis_index("w")
        hi = lax.axis_index("h")
        me = hi * 4 + wi
        barrier = pltpu.get_barrier_semaphore()

        def peer(k):
            d = lax.rem(me + k, 16)
            return d, {"h": d // 4, "w": lax.rem(d, 4)}

        for k in range(1, 16):
            pl.semaphore_signal(barrier, inc=1, device_id=peer(k)[1], device_id_type=MESH)

        side = wi // 2
        twin = 2 * hi + lax.rem(wi, 2)

        def first_image(p, h, w):
            solo = 2 * SOLO * (4 * h + w) + 2 * p
            shared = 2 * SOLO * 16 + 2 * (PAIRS - SOLO) * (2 * h + lax.rem(w, 2)) + 2 * (p - SOLO)
            return jnp.where(p < SOLO, solo, shared) if not isinstance(p, int) else (solo if p < SOLO else shared)

        r, c = iota((32, BLOCK), 0), iota((32, BLOCK), 1)
        pmat[...] = ((c // 16 == r % 16) & ((c // 2) % 2 == r // 16)).astype(F32).astype(BF)
        r, c = iota((LANE, BLOCK), 0) // 16, iota((LANE, BLOCK), 1)
        lanes[...] = (((c // 4) % 4 == r // 2) & (c % 2 == r % 2)).astype(F32).astype(BF)

        def pack(ch):
            def step(t, carry):
                wide = []
                for k in (2 * t, 2 * t + 1):
                    dev = peer(k)[1]
                    at = pl.multiple_of(8 * first_image(ch, dev["h"], dev["w"]), 16)
                    wide.append(jnp.concatenate([x_ref[pl.ds(at, 16), :]] * 8, axis=0) * lanes[...])
                turned = lax.dot_general(pmat[...], jnp.concatenate(wide, axis=0), (((1,), (1,)), ((), ())),
                                         preferred_element_type=F32).astype(BF)
                slab[ch, 2 * t] = turned[:, :LANE]
                slab[ch, 2 * t + 1] = turned[:, LANE:]
                return carry
            lax.fori_loop(0, 8, step, 0)

        def send(ch):
            def step(k, carry):
                pltpu.make_async_remote_copy(
                    src_ref=slab.at[ch, k], dst_ref=recv.at[ch, me], send_sem=send_in, recv_sem=recv_in.at[ch],
                    device_id=peer(k)[1], device_id_type=MESH).start()
                return carry
            lax.fori_loop(1, 16, step, 0)
            recv[ch, me] = slab[ch, 0]

        loads[0].wait()
        pack(0)
        pl.semaphore_wait(barrier, 15)
        send(0)
        for ch in range(1, 3):
            pack(ch)
            send(ch)

        for load in loads[1:]:
            load.wait()
        r, c = iota((512, WIDE), 0), iota((512, WIDE), 1)
        column = (r // LANE == (c // 8) % 4) & (r % 8 == c % 8) & ((r // 32) % 4 == c // BLOCK)
        here = (c % BLOCK < LANE) & ((c // 64) % 2 == (r // 8) % 2) & ((c // 32) % 2 == (r // 16) % 2)
        above = (c % BLOCK >= LANE) & (c % LANE < 64) & ((c // 32) % 2 == (r // 8) % 2) & ((r // 16) % 2 == 1)
        smat[...] = (column & (here | above)).astype(F32).astype(BF)
        r, c = iota((384, LANE), 0) % LANE, iota((384, LANE), 1)
        for s, chan in enumerate((64, LANE, BLOCK)):
            size = chan // 8
            gmat[s] = ((r % chan) // size == (c % chan) // size).astype(F32).astype(BF)
        for s, v in enumerate((v1d, v1r, v2d, v2r, v3d, v3r)):
            chan = CHANS[s]
            if chan == 64:
                aff[s, 0:3, :] = jnp.concatenate([v[...], v[...]], axis=1)
            else:
                aff[s, 0:3, :] = v[:, 0:LANE]
                if chan == BLOCK:
                    aff[s, 3:6, :] = v[:, LANE:BLOCK]
        t1[...] = jnp.zeros_like(t1)
        row, col = iota((32, WIDE), 0), iota((32, WIDE), 1) // 64
        for dh in range(3):
            base = jnp.zeros((32, WIDE), F32)
            for dw in range(3):
                tap = w1d[dh, dw:dw + 1, :].astype(F32)
                tap = jnp.concatenate([tap, tap], axis=1)
                tap = jnp.concatenate([tap] * 8, axis=1)
                base = jnp.where(row == 2 * col + dw - 1, jnp.broadcast_to(tap, (32, WIDE)), base)
            for i in range(2):
                at = LANE + 32 * i if dh == 0 else 64 * i + 32 * (dh - 1)
                t1[i, at:at + 32, :] = base.astype(BF)
        tr1[...] = jnp.zeros_like(tr1)
        td2[...] = jnp.zeros_like(td2)
        tr2[...] = jnp.zeros_like(tr2)
        for dh in range(3):
            for dw in range(3):
                tap = w1r[dh, 64 * dw:64 * dw + 64, :]
                for jo in range(4):
                    ji = jo + 1 + dw
                    tr1[dh, 64 * ji:64 * ji + 64, 64 * jo:64 * jo + 64] = tap
                tap = w2d[dh, 64 * dw:64 * dw + 64, :]
                for jo in range(2):
                    ji = 2 * jo + 1 + dw
                    td2[dh, 64 * ji:64 * ji + 64, LANE * jo:LANE * jo + LANE] = tap
                tap = w2r[dh, LANE * dw:LANE * dw + LANE, :]
                for jo in range(2):
                    ji = jo + dw
                    tr2[dh, LANE * ji:LANE * ji + LANE, LANE * jo:LANE * jo + LANE] = tap
        for ch in range(3, PAIRS):
            pack(ch)
            send(ch)

        top = iota((64, BLOCK), 0) == 0
        bottom = iota((64, BLOCK), 0) == 63

        def taps(ref, j, rows, stride, lo, hi_, h0, h1):
            pieces = []
            for dh in range(3):
                if stride == 1:
                    piece = ref[j, h0:h1, dh:dh + rows, :, lo:hi_]
                    pieces.append(piece.reshape((h1 - h0) * 16 * rows, hi_ - lo))
                else:
                    pieces.append(jnp.concatenate(
                        [ref[j, h, 2 * l + dh, :, lo:hi_] for h in range(h0, h1) for l in range(rows)], axis=0))
            return jnp.concatenate(pieces, axis=1)

        def conv(j, s, b, i):
            rows = ROWS[s]
            lo = BLOCK * b
            step = min(4, CHUNK // (16 * rows))
            sums = sqs = None
            for h0 in range(0, 4, step):
                h1 = h0 + step
                m = 16 * rows * step
                if s == 0:
                    lhs = zin[h0:h1, 0:8].reshape(m, BLOCK)
                    rhs = t1[i, :, lo:lo + BLOCK]
                elif s in (1, 3):
                    ref, mat = ((zd1, tr1), (zd2, tr2))[s // 2]
                    first, last = (LANE if b == 0 else 0), (384 if b == 3 else 512)
                    lhs = taps(ref, j, rows, 1, lo - LANE + first, lo - LANE + last, h0, h1)
                    rhs = mat[:, first:last, :].reshape(3 * (last - first), BLOCK)
                elif s in (2, 4):
                    ref, mat = ((zr1, td2), (zr2, w3d))[s // 2 - 1]
                    first = LANE if b == 0 else 0
                    lhs = taps(ref, j, rows, 2, lo - LANE + first, lo + BLOCK, h0, h1)
                    rhs = mat[:, first:384, :].reshape(3 * (384 - first), BLOCK)
                else:
                    first, last = (BLOCK if b == 0 else 0), (512 if b == 3 else 768)
                    lhs = taps(zd3, j, rows, 1, lo - BLOCK + first, lo - BLOCK + last, h0, h1)
                    rhs = w3r[:, first:last, :].reshape(3 * (last - first), BLOCK)
                out = jnp.dot(lhs, rhs, preferred_element_type=F32)
                at = 16 * rows * h0
                acc[j, at:at + m, lo:lo + BLOCK] = out
                tall = out.reshape(m // 8, 8, BLOCK)
                one, two = jnp.sum(tall, axis=0), jnp.sum(tall * tall, axis=0)
                sums, sqs = (one, two) if sums is None else (sums + one, sqs + two)
            return sums, sqs

        def finish(s, parts):
            m, chan = 64 * ROWS[s], CHANS[s]
            sums = parts[0][0] + parts[1][0] + parts[2][0] + parts[3][0]
            sqs = parts[0][1] + parts[1][1] + parts[2][1] + parts[3][1]
            if chan == BLOCK:
                sides, per_lane = [(sums[:, 0:LANE], sqs[:, 0:LANE]), (sums[:, LANE:], sqs[:, LANE:])], 4.0 * m
            else:
                sides, per_lane = [(sums[:, 0:LANE] + sums[:, LANE:], sqs[:, 0:LANE] + sqs[:, LANE:])], 8.0 * m
            count = float(m * WIDE // 8)
            row16 = iota((16, LANE), 0)
            packed = jnp.zeros((16, LANE), F32)
            for n, (one, two) in enumerate(sides):
                bias = aff[s, 3 * n:3 * n + 1, :]
                one = jnp.sum(one, axis=0, keepdims=True)
                two = jnp.sum(two, axis=0, keepdims=True)
                total = one + per_lane * bias
                square = two + bias * (one + total)
                packed = jnp.where(row16 == 2 * n, total, jnp.where(row16 == 2 * n + 1, square, packed))
            high = packed.astype(BF)
            rest = packed - high.astype(F32)
            mid = rest.astype(BF)
            low = (rest - mid.astype(F32)).astype(BF)
            totals = jnp.dot(jnp.concatenate([high, mid, low], axis=1), gmat[s // 2], preferred_element_type=F32)
            scales, shifts = [], []
            for n in range(len(sides)):
                bias, gain, beta = (aff[s, 3 * n + t:3 * n + t + 1, :] for t in range(3))
                mean = totals[2 * n:2 * n + 1] * (1.0 / count)
                var = jnp.maximum(totals[2 * n + 1:2 * n + 2] * (1.0 / count) - mean * mean, 0.0)
                scale = lax.rsqrt(var + NORM_EPS) * gain
                scales.append(scale)
                shifts.append(beta + (bias - mean) * scale)
            if len(sides) == 1:
                scales, shifts = scales * 2, shifts * 2
            return jnp.concatenate(scales, axis=1), jnp.concatenate(shifts, axis=1)

        def norm(j, s, b, affine):
            rows = ROWS[s]
            m = 64 * rows
            lo = BLOCK * b
            z = jnp.maximum(acc[j, 0:m, lo:lo + BLOCK] * affine[0] + affine[1], 0.0).reshape(4, rows, 16, BLOCK)
            if s == 5:
                for h in range(4):
                    for l in range(2):
                        for t in range(2):
                            fst[j, 2 * (4 * h + b) + t, pl.ds(l, 16, stride=2), :] = z[h, l, :, LANE * t:LANE * t + LANE]
                return
            ref = (zd1, zr1, zd2, zr2, zd3)[s]
            ref[j, :, 1:1 + rows, :, lo:lo + BLOCK] = z.astype(BF)
            edge = pltpu.roll(z[:, rows - 1].reshape(64, BLOCK), 1, axis=0)
            ref[j, :, 0, :, lo:lo + BLOCK] = jnp.where(top, 0.0, edge).reshape(4, 16, BLOCK).astype(BF)
            if s in (0, 2, 4):
                edge = pltpu.roll(z[:, 0].reshape(64, BLOCK), 63, axis=0)
                ref[j, :, 1 + rows, :, lo:lo + BLOCK] = jnp.where(bottom, 0.0, edge).reshape(4, 16, BLOCK).astype(BF)

        def out_copy(p, d):
            h, w = d // 4, lax.rem(d, 4)
            return pltpu.make_async_remote_copy(
                src_ref=outb.at[d, pl.ds(2 * p, 2)], dst_ref=o_ref.at[pl.ds(first_image(p, hi, wi), 2)],
                send_sem=send_out, recv_sem=recv_out, device_id={"h": h, "w": w}, device_id_type=MESH)

        def emit(j, n):
            for d in range(16):
                outb[d, n] = jnp.concatenate([fst[j, 2 * d], fst[j, 2 * d + 1]], axis=1).astype(BF)

        def pair(p, carry):
            pltpu.make_async_copy(recv.at[p, 0:15], recv.at[p, 0:15], recv_in.at[p]).wait()
            wide = jnp.concatenate([
                jnp.concatenate([recv[p, 4 * h + w] for h in range(4)], axis=0) for w in range(4)], axis=1)
            spread = jnp.dot(wide, smat[...], preferred_element_type=F32)
            for lq in range(4):
                here, above = (spread[:, LANE * t:LANE * t + LANE].reshape(4, 2, 16, LANE) for t in (2 * lq, 2 * lq + 1))
                zin[:, 2 * lq:2 * lq + 2, :, :LANE] = here.astype(BF)
                zin[:, 2 * lq + 1:2 * lq + 3, :, LANE:] = above.astype(BF)
            edge = pltpu.roll(above[:, 1].reshape(64, LANE), 1, axis=0)
            edge = jnp.where(iota((64, LANE), 0) == 0, 0.0, edge)
            zin[:, 0, :, LANE:] = edge.astype(BF).reshape(4, 16, LANE)

            waiting = None
            for s in range(6):
                for j in range(2):
                    parts = []
                    for b in range(4):
                        parts.append(conv(j, s, b, j))
                        if waiting is not None:
                            norm(*waiting[0:2], b, waiting[2])
                    waiting = (j, s, finish(s, parts))

            @pl.when(p < PAIRS)
            def _():
                emit(0, 2 * p)

            for b in range(4):
                norm(*waiting[0:2], b, waiting[2])
            emit(1, 2 * p + 1)

            @pl.when(p < SOLO)
            def _():
                for k in range(1, 16):
                    out_copy(p, peer(k)[0]).start()

            @pl.when(p >= SOLO)
            def _():
                for k in range(1, 8):
                    t = lax.rem(twin + k, 8)
                    out_copy(p, 4 * (t // 2) + 2 * side + lax.rem(t, 2)).start()

            return carry

        lax.fori_loop(0, PAIRS, pair, 0)

        for at, size, base in ((0, 2 * SOLO, first_image(0, hi, wi)), (2 * SOLO, 2 * (PAIRS - SOLO), first_image(SOLO, hi, wi))):
            own = pltpu.make_async_copy(outb.at[me, at:at + size], o_ref.at[pl.ds(base, size)], local_out)
            own.start()
            own.wait()
        pltpu.make_async_copy(slab.at[:, 0:15], slab.at[:, 0:15], send_in).wait()
        moved = o_ref.at[0:count - 2 * PAIRS]
        pltpu.make_async_copy(moved, moved, send_out).wait()
        pltpu.make_async_copy(moved, moved, recv_out).wait()

    return kernel


def encode(tile, params):
    count = tile.shape[0]
    rows = tile.reshape(count, BLOCK, 8).transpose(0, 2, 1).reshape(count * 8, BLOCK)
    weights = []
    for n, param in enumerate(params):
        if n == 0:
            weights.append(param.reshape(3, 3, 64))
        elif n % 2 == 0:
            weights.append(param.reshape(3, 3 * param.shape[2], param.shape[3]))
        else:
            weights.append(param)
    operands = [rows, *weights]
    return pl.pallas_call(
        make_kernel(count),
        out_shape=jax.ShapeDtypeStruct((count, 32, BLOCK), BF),
        in_specs=[pl.BlockSpec(memory_space=pltpu.HBM)] * ARGS,
        out_specs=pl.BlockSpec(memory_space=pl.ANY),
        scratch_shapes=[pltpu.VMEM(a.shape, a.dtype) for a in operands] + [
            pltpu.SemaphoreType.DMA((ARGS,)),
            pltpu.VMEM((PAIRS, 16, 32, LANE), BF),
            pltpu.VMEM((PAIRS, 16, 32, LANE), BF),
            pltpu.VMEM((4, 9, 16, BLOCK), BF),
            pltpu.VMEM((2, BLOCK, WIDE), BF),
            pltpu.VMEM((3, 512, BLOCK), BF),
            pltpu.VMEM((3, 384, BLOCK), BF),
            pltpu.VMEM((3, 512, BLOCK), BF),
            pltpu.VMEM((6, 8, LANE), F32),
            pltpu.VMEM((3, 384, LANE), BF),
            pltpu.VMEM((512, WIDE), BF),
            pltpu.VMEM((32, BLOCK), BF),
            pltpu.VMEM((LANE, BLOCK), BF),
            pltpu.VMEM((2, 512, WIDE), F32),
            pltpu.VMEM((2, 4, 10, 16, WIDE), BF),
            pltpu.VMEM((2, 4, 9, 16, WIDE), BF),
            pltpu.VMEM((2, 4, 6, 16, WIDE), BF),
            pltpu.VMEM((2, 4, 5, 16, WIDE), BF),
            pltpu.VMEM((2, 4, 4, 16, WIDE), BF),
            pltpu.VMEM((2, 32, 32, LANE), F32),
            pltpu.VMEM((16, 2 * PAIRS, 32, BLOCK), BF),
            pltpu.SemaphoreType.DMA,
            pltpu.SemaphoreType.DMA((PAIRS,)),
            pltpu.SemaphoreType.DMA,
            pltpu.SemaphoreType.DMA,
            pltpu.SemaphoreType.DMA,
        ],
        compiler_params=pltpu.CompilerParams(
            collective_id=0, has_side_effects=True, vmem_limit_bytes=57 * WIDE * WIDE),
        name="encoder",
    )(*operands)


def solution(mesh):
    act_spec = P("batch", "h", "w")

    def local_forward(tile, *params):
        return encode(tile, params)[:, :, None, :]

    return jax.shard_map(local_forward, mesh=mesh, in_specs=(act_spec,) + (P(),) * 12, out_specs=act_spec, check_vma=False)
```

```python
import jax
import jax.numpy as jnp
from jax import lax
from jax.experimental import pallas as pl
from jax.experimental.pallas import tpu as pltpu
from jax.sharding import PartitionSpec as P

NORM_EPS = 1e-5
HALF = 64
LANE = 128
BLOCK = 256
WIDE = 1024
CHUNK = 512
PAIRS = 7
SOLO = 5
ARGS = 13
BF = jnp.bfloat16
F32 = jnp.float32
MESH = pl.DeviceIdType.MESH
ROWS = (8, 8, 4, 4, 2, 2)
CHANS = (64, 64, 128, 128, 256, 256)


def iota(shape, axis):
    return lax.broadcasted_iota(jnp.int32, shape, axis)


def make_kernel(count):
    def kernel(*refs):
        inputs, (o_ref, *refs) = refs[:ARGS], refs[ARGS:]
        local, refs = refs[:ARGS], refs[ARGS:]
        body(inputs, local, o_ref, *refs)

    def body(inputs, local, o_ref, load_sem,
               slab, recv, zin, t1, tr1, td2, tr2, aff, gmat, smat, pmat, lanes,
               acc, zd1, zr1, zd2, zr2, zd3, fst, outb,
               send_in, recv_in, send_out, recv_out, local_out):
        x_ref, w1d, v1d, w1r, v1r, w2d, v2d, w2r, v2r, w3d, v3d, w3r, v3r = local
        loads = [pltpu.make_async_copy(inputs[n], local[n], load_sem.at[n]) for n in range(ARGS)]
        for load in loads:
            load.start()
        wi = lax.axis_index("w")
        hi = lax.axis_index("h")
        me = hi * 4 + wi
        barrier = pltpu.get_barrier_semaphore()

        def peer(k):
            d = lax.rem(me + k, 16)
            return d, {"h": d // 4, "w": lax.rem(d, 4)}

        for k in range(1, 16):
            pl.semaphore_signal(barrier, inc=1, device_id=peer(k)[1], device_id_type=MESH)

        side = wi // 2
        twin = 2 * hi + lax.rem(wi, 2)

        def first_image(p, h, w):
            solo = 2 * SOLO * (4 * h + w) + 2 * p
            shared = 2 * SOLO * 16 + 2 * (PAIRS - SOLO) * (2 * h + lax.rem(w, 2)) + 2 * (p - SOLO)
            return jnp.where(p < SOLO, solo, shared) if not isinstance(p, int) else (solo if p < SOLO else shared)

        r, c = iota((32, BLOCK), 0), iota((32, BLOCK), 1)
        pmat[...] = ((c // 16 == r % 16) & ((c // 2) % 2 == r // 16)).astype(F32).astype(BF)
        r, c = iota((LANE, BLOCK), 0) // 16, iota((LANE, BLOCK), 1)
        lanes[...] = (((c // 4) % 4 == r // 2) & (c % 2 == r % 2)).astype(F32).astype(BF)

        def pack(ch):
            def step(t, carry):
                wide = []
                for k in (2 * t, 2 * t + 1):
                    dev = peer(k)[1]
                    at = pl.multiple_of(8 * first_image(ch, dev["h"], dev["w"]), 16)
                    wide.append(jnp.concatenate([x_ref[pl.ds(at, 16), :]] * 8, axis=0) * lanes[...])
                turned = lax.dot_general(pmat[...], jnp.concatenate(wide, axis=0), (((1,), (1,)), ((), ())),
                                         preferred_element_type=F32).astype(BF)
                slab[ch, 2 * t] = turned[:, :LANE]
                slab[ch, 2 * t + 1] = turned[:, LANE:]
                return carry
            lax.fori_loop(0, 8, step, 0)

        def send(ch):
            def step(k, carry):
                pltpu.make_async_remote_copy(
                    src_ref=slab.at[ch, k], dst_ref=recv.at[ch, me], send_sem=send_in, recv_sem=recv_in.at[ch],
                    device_id=peer(k)[1], device_id_type=MESH).start()
                return carry
            lax.fori_loop(1, 16, step, 0)
            recv[ch, me] = slab[ch, 0]

        loads[0].wait()
        pack(0)
        pl.semaphore_wait(barrier, 15)
        send(0)
        for ch in range(1, 3):
            pack(ch)
            send(ch)

        for load in loads[1:]:
            load.wait()
        r, c = iota((512, WIDE), 0), iota((512, WIDE), 1)
        column = (r // LANE == (c // 8) % 4) & (r % 8 == c % 8) & ((r // 32) % 4 == c // BLOCK)
        here = (c % BLOCK < LANE) & ((c // HALF) % 2 == (r // 8) % 2) & ((c // 32) % 2 == (r // 16) % 2)
        above = (c % BLOCK >= LANE) & (c % LANE < HALF) & ((c // 32) % 2 == (r // 8) % 2) & ((r // 16) % 2 == 1)
        smat[...] = (column & (here | above)).astype(F32).astype(BF)
        r, c = iota((384, LANE), 0) % LANE, iota((384, LANE), 1)
        for s, chan in enumerate((HALF, LANE, BLOCK)):
            size = chan // 8
            gmat[s] = ((r % chan) // size == (c % chan) // size).astype(F32).astype(BF)
        for s, v in enumerate((v1d, v1r, v2d, v2r, v3d, v3r)):
            chan = CHANS[s]
            if chan == HALF:
                aff[s, 0:3, :] = jnp.concatenate([v[...], v[...]], axis=1)
            else:
                aff[s, 0:3, :] = v[:, 0:LANE]
                if chan == BLOCK:
                    aff[s, 3:6, :] = v[:, LANE:BLOCK]
        t1[...] = jnp.zeros_like(t1)
        row, col = iota((32, WIDE), 0), iota((32, WIDE), 1) // HALF
        for dh in range(3):
            base = jnp.zeros((32, WIDE), F32)
            for dw in range(3):
                tap = w1d[dh, dw:dw + 1, :].astype(F32)
                tap = jnp.concatenate([tap, tap], axis=1)
                tap = jnp.concatenate([tap] * 8, axis=1)
                base = jnp.where(row == 2 * col + dw - 1, jnp.broadcast_to(tap, (32, WIDE)), base)
            for i in range(2):
                at = LANE + 32 * i if dh == 0 else HALF * i + 32 * (dh - 1)
                t1[i, at:at + 32, :] = base.astype(BF)
        tr1[...] = jnp.zeros_like(tr1)
        td2[...] = jnp.zeros_like(td2)
        tr2[...] = jnp.zeros_like(tr2)
        for dh in range(3):
            for dw in range(3):
                tap = w1r[dh, HALF * dw:HALF * dw + HALF, :]
                for t in range(2):
                    for jo in range(2):
                        row = BLOCK * (dh + t) + HALF * ((jo + dw + 3) % 4)
                        col = LANE * t + HALF * jo
                        tr1[row:row + HALF, col:col + HALF] = tap
                tap = w2d[dh, HALF * dw:HALF * dw + HALF, :]
                for jo in range(2):
                    ji = 2 * jo + 1 + dw
                    td2[dh, HALF * ji:HALF * ji + HALF, LANE * jo:LANE * jo + LANE] = tap
                tap = w2r[dh, LANE * dw:LANE * dw + LANE, :]
                for jo in range(2):
                    ji = jo + dw
                    tr2[dh, LANE * ji:LANE * ji + LANE, LANE * jo:LANE * jo + LANE] = tap
        for ch in range(3, PAIRS):
            pack(ch)
            send(ch)

        top = iota((HALF, BLOCK), 0) == 0
        bottom = iota((HALF, BLOCK), 0) == 63

        def taps(ref, j, rows, stride, lo, hi_, h0, h1):
            pieces = []
            for dh in range(3):
                if stride == 1:
                    piece = ref[j, h0:h1, dh:dh + rows, :, lo:hi_]
                    pieces.append(piece.reshape((h1 - h0) * 16 * rows, hi_ - lo))
                else:
                    pieces.append(jnp.concatenate(
                        [ref[j, h, 2 * l + dh, :, lo:hi_] for h in range(h0, h1) for l in range(rows)], axis=0))
            return jnp.concatenate(pieces, axis=1)

        def conv_square(j, b):
            sums = sqs = 0.0
            for p in (2 * b, 2 * b + 1):
                pieces = []
                for t in range(4):
                    for lo in (LANE * p, WIDE + LANE * p):
                        pieces.append(jnp.concatenate(
                            [zd1[j, h, 2 * l + t, :, lo:lo + LANE] for h in range(4) for l in range(4)], axis=0))
                out = jnp.dot(jnp.concatenate(pieces, axis=1), tr1[...], preferred_element_type=F32)
                tall = out.reshape(BLOCK // 8, 8, BLOCK)
                sums, sqs = sums + jnp.sum(tall, axis=0), sqs + jnp.sum(tall * tall, axis=0)
                out = out.reshape(16, 16, BLOCK)
                for n in range(16):
                    for t in range(2):
                        at = 16 * (2 * n + t)
                        acc[j, at:at + 16, LANE * p:LANE * p + LANE] = out[n, :, LANE * t:LANE * t + LANE]
            return sums, sqs

        def conv(j, s, b, i):
            rows = ROWS[s]
            lo = BLOCK * b
            if s == 1:
                return conv_square(j, b)
            step = min(4, CHUNK // (16 * rows))
            sums = sqs = None
            for h0 in range(0, 4, step):
                h1 = h0 + step
                m = 16 * rows * step
                if s == 0:
                    lhs = zin[h0:h1, 0:8].reshape(m, BLOCK)
                    rhs = t1[i, :, lo:lo + BLOCK]
                elif s == 3:
                    ref, mat = zd2, tr2
                    first, last = (LANE if b == 0 else 0), (384 if b == 3 else 512)
                    lhs = taps(ref, j, rows, 1, lo - LANE + first, lo - LANE + last, h0, h1)
                    rhs = mat[:, first:last, :].reshape(3 * (last - first), BLOCK)
                elif s in (2, 4):
                    ref, mat = ((zr1, td2), (zr2, w3d))[s // 2 - 1]
                    first = LANE if b == 0 else 0
                    lhs = taps(ref, j, rows, 2, lo - LANE + first, lo + BLOCK, h0, h1)
                    rhs = mat[:, first:384, :].reshape(3 * (384 - first), BLOCK)
                else:
                    first, last = (BLOCK if b == 0 else 0), (512 if b == 3 else 768)
                    lhs = taps(zd3, j, rows, 1, lo - BLOCK + first, lo - BLOCK + last, h0, h1)
                    rhs = w3r[:, first:last, :].reshape(3 * (last - first), BLOCK)
                out = jnp.dot(lhs, rhs, preferred_element_type=F32)
                at = 16 * rows * h0
                acc[j, at:at + m, lo:lo + BLOCK] = out
                tall = out.reshape(m // 8, 8, BLOCK)
                one, two = jnp.sum(tall, axis=0), jnp.sum(tall * tall, axis=0)
                sums, sqs = (one, two) if sums is None else (sums + one, sqs + two)
            return sums, sqs

        def finish(s, parts):
            m, chan = HALF * ROWS[s], CHANS[s]
            sums = parts[0][0] + parts[1][0] + parts[2][0] + parts[3][0]
            sqs = parts[0][1] + parts[1][1] + parts[2][1] + parts[3][1]
            if chan == BLOCK:
                sides, per_lane = [(sums[:, 0:LANE], sqs[:, 0:LANE]), (sums[:, LANE:], sqs[:, LANE:])], 4.0 * m
            else:
                sides, per_lane = [(sums[:, 0:LANE] + sums[:, LANE:], sqs[:, 0:LANE] + sqs[:, LANE:])], 8.0 * m
            count = float(m * WIDE // 8)
            row16 = iota((16, LANE), 0)
            packed = jnp.zeros((16, LANE), F32)
            for n, (one, two) in enumerate(sides):
                bias = aff[s, 3 * n:3 * n + 1, :]
                one = jnp.sum(one, axis=0, keepdims=True)
                two = jnp.sum(two, axis=0, keepdims=True)
                total = one + per_lane * bias
                square = two + bias * (one + total)
                packed = jnp.where(row16 == 2 * n, total, jnp.where(row16 == 2 * n + 1, square, packed))
            high = packed.astype(BF)
            rest = packed - high.astype(F32)
            mid = rest.astype(BF)
            low = (rest - mid.astype(F32)).astype(BF)
            totals = jnp.dot(jnp.concatenate([high, mid, low], axis=1), gmat[s // 2], preferred_element_type=F32)
            scales, shifts = [], []
            for n in range(len(sides)):
                bias, gain, beta = (aff[s, 3 * n + t:3 * n + t + 1, :] for t in range(3))
                mean = totals[2 * n:2 * n + 1] * (1.0 / count)
                var = jnp.maximum(totals[2 * n + 1:2 * n + 2] * (1.0 / count) - mean * mean, 0.0)
                scale = lax.rsqrt(var + NORM_EPS) * gain
                scales.append(scale)
                shifts.append(beta + (bias - mean) * scale)
            if len(sides) == 1:
                scales, shifts = scales * 2, shifts * 2
            return jnp.concatenate(scales, axis=1), jnp.concatenate(shifts, axis=1)

        def norm(j, s, b, affine):
            rows = ROWS[s]
            m = HALF * rows
            lo = BLOCK * b
            z = jnp.maximum(acc[j, 0:m, lo:lo + BLOCK] * affine[0] + affine[1], 0.0).reshape(4, rows, 16, BLOCK)
            if s == 5:
                for h in range(4):
                    for l in range(2):
                        for t in range(2):
                            fst[j, 2 * (4 * h + b) + t, pl.ds(l, 16, stride=2), :] = z[h, l, :, LANE * t:LANE * t + LANE]
                return
            ref = (zd1, zr1, zd2, zr2, zd3)[s]
            ref[j, :, 1:1 + rows, :, lo:lo + BLOCK] = z.astype(BF)
            edge = pltpu.roll(z[:, rows - 1].reshape(HALF, BLOCK), 1, axis=0)
            ref[j, :, 0, :, lo:lo + BLOCK] = jnp.where(top, 0.0, edge).reshape(4, 16, BLOCK).astype(BF)
            if s % 2 == 0:
                edge = pltpu.roll(z[:, 0].reshape(HALF, BLOCK), 63, axis=0)
                ref[j, :, 1 + rows, :, lo:lo + BLOCK] = jnp.where(bottom, 0.0, edge).reshape(4, 16, BLOCK).astype(BF)
            if s == 0:
                for p in range(max(2 * b - 1, 0), 2 * b + 1 + b // 3):
                    left = zd1[j, :, :, :, LANE * p - LANE:LANE * p] if p > 0 else jnp.zeros((4, 10, 16, LANE), BF)
                    right = zd1[j, :, :, :, LANE * p + LANE:LANE * p + BLOCK] if p < 7 else jnp.zeros((4, 10, 16, LANE), BF)
                    zd1[j, :, :, :, WIDE + LANE * p:WIDE + LANE * p + LANE] = jnp.where(
                        iota((4, 10, 16, LANE), 3) < HALF, right, left)

        def out_copy(p, d):
            h, w = d // 4, lax.rem(d, 4)
            return pltpu.make_async_remote_copy(
                src_ref=outb.at[d, pl.ds(2 * p, 2)], dst_ref=o_ref.at[pl.ds(first_image(p, hi, wi), 2)],
                send_sem=send_out, recv_sem=recv_out, device_id={"h": h, "w": w}, device_id_type=MESH)

        def emit(j, n):
            for d in range(16):
                outb[d, n] = jnp.concatenate([fst[j, 2 * d], fst[j, 2 * d + 1]], axis=1).astype(BF)

        def pair(p, carry):
            pltpu.make_async_copy(recv.at[p, 0:15], recv.at[p, 0:15], recv_in.at[p]).wait()
            wide = jnp.concatenate([
                jnp.concatenate([recv[p, 4 * h + w] for h in range(4)], axis=0) for w in range(4)], axis=1)
            spread = jnp.dot(wide, smat[...], preferred_element_type=F32)
            for lq in range(4):
                here, above = (spread[:, LANE * t:LANE * t + LANE].reshape(4, 2, 16, LANE) for t in (2 * lq, 2 * lq + 1))
                zin[:, 2 * lq:2 * lq + 2, :, :LANE] = here.astype(BF)
                zin[:, 2 * lq + 1:2 * lq + 3, :, LANE:] = above.astype(BF)
            edge = pltpu.roll(above[:, 1].reshape(HALF, LANE), 1, axis=0)
            edge = jnp.where(iota((HALF, LANE), 0) == 0, 0.0, edge)
            zin[:, 0, :, LANE:] = edge.astype(BF).reshape(4, 16, LANE)

            waiting = None
            for s in range(6):
                for j in range(2):
                    parts = []
                    for b in range(4):
                        parts.append(conv(j, s, b, j))
                        if waiting is not None:
                            norm(*waiting[0:2], b, waiting[2])
                    waiting = (j, s, finish(s, parts))
                    if (s, j) in ((0, 0), (0, 1)):
                        @pl.when(p < PAIRS)
                        def _():
                            aff[0, 7:8, :] = aff[0, 0:1, :]

            @pl.when(p < PAIRS)
            def _():
                emit(0, 2 * p)

            for b in range(4):
                norm(*waiting[0:2], b, waiting[2])
            emit(1, 2 * p + 1)

            @pl.when(p < SOLO)
            def _():
                for k in range(1, 16):
                    out_copy(p, peer(k)[0]).start()

            @pl.when(p >= SOLO)
            def _():
                for k in range(1, 8):
                    t = lax.rem(twin + k, 8)
                    out_copy(p, 4 * (t // 2) + 2 * side + lax.rem(t, 2)).start()

            return carry

        lax.fori_loop(0, PAIRS, pair, 0)

        for at, size, base in ((0, 2 * SOLO, first_image(0, hi, wi)), (2 * SOLO, 2 * (PAIRS - SOLO), first_image(SOLO, hi, wi))):
            own = pltpu.make_async_copy(outb.at[me, at:at + size], o_ref.at[pl.ds(base, size)], local_out)
            own.start()
            own.wait()
        pltpu.make_async_copy(slab.at[:, 0:15], slab.at[:, 0:15], send_in).wait()
        moved = o_ref.at[0:count - 2 * PAIRS]
        pltpu.make_async_copy(moved, moved, send_out).wait()
        pltpu.make_async_copy(moved, moved, recv_out).wait()

    return kernel


def encode(tile, params):
    count = tile.shape[0]
    rows = tile.reshape(count, BLOCK, 8).transpose(0, 2, 1).reshape(count * 8, BLOCK)
    weights = []
    for n, param in enumerate(params):
        if n == 0:
            weights.append(param.reshape(3, 3, HALF))
        elif n % 2 == 0:
            weights.append(param.reshape(3, 3 * param.shape[2], param.shape[3]))
        else:
            weights.append(param)
    operands = [rows, *weights]
    return pl.pallas_call(
        make_kernel(count),
        out_shape=jax.ShapeDtypeStruct((count, 32, BLOCK), BF),
        in_specs=[pl.BlockSpec(memory_space=pltpu.HBM)] * ARGS,
        out_specs=pl.BlockSpec(memory_space=pl.ANY),
        scratch_shapes=[pltpu.VMEM(a.shape, a.dtype) for a in operands] + [
            pltpu.SemaphoreType.DMA((ARGS,)),
            pltpu.VMEM((PAIRS, 16, 32, LANE), BF),
            pltpu.VMEM((PAIRS, 16, 32, LANE), BF),
            pltpu.VMEM((4, 9, 16, BLOCK), BF),
            pltpu.VMEM((2, BLOCK, WIDE), BF),
            pltpu.VMEM((WIDE, BLOCK), BF),
            pltpu.VMEM((3, 384, BLOCK), BF),
            pltpu.VMEM((3, 512, BLOCK), BF),
            pltpu.VMEM((6, 8, LANE), F32),
            pltpu.VMEM((3, 384, LANE), BF),
            pltpu.VMEM((512, WIDE), BF),
            pltpu.VMEM((32, BLOCK), BF),
            pltpu.VMEM((LANE, BLOCK), BF),
            pltpu.VMEM((2, 512, WIDE), F32),
            pltpu.VMEM((2, 4, 10, 16, 2 * WIDE), BF),
            pltpu.VMEM((2, 4, 9, 16, WIDE), BF),
            pltpu.VMEM((2, 4, 6, 16, WIDE), BF),
            pltpu.VMEM((2, 4, 5, 16, WIDE), BF),
            pltpu.VMEM((2, 4, 4, 16, WIDE), BF),
            pltpu.VMEM((2, 32, 32, LANE), F32),
            pltpu.VMEM((16, 2 * PAIRS, 32, BLOCK), BF),
            pltpu.SemaphoreType.DMA,
            pltpu.SemaphoreType.DMA((PAIRS,)),
            pltpu.SemaphoreType.DMA,
            pltpu.SemaphoreType.DMA,
            pltpu.SemaphoreType.DMA,
        ],
        compiler_params=pltpu.CompilerParams(
            collective_id=0, has_side_effects=True, vmem_limit_bytes=58 * WIDE * WIDE),
        name="encoder",
    )(*operands)


def solution(mesh):
    act_spec = P("batch", "h", "w")

    def local_forward(tile, *params):
        return encode(tile, params)[:, :, None, :]

    return jax.shard_map(local_forward, mesh=mesh, in_specs=(act_spec,) + (P(),) * 12, out_specs=act_spec, check_vma=False)
```

```python
import jax
import jax.numpy as jnp
from jax import lax
from jax.experimental import pallas as pl
from jax.experimental.pallas import tpu as pltpu
from jax.sharding import PartitionSpec as P

NORM_EPS = 1e-5
LANE = 128
BLOCK = 256
WIDE = 1024
CHUNK = 512
PAIRS = 7
SOLO = 5
GROUPS = ((0, 1), (1, 2), (3, 4))
ARGS = 13
BF = jnp.bfloat16
F32 = jnp.float32
MESH = pl.DeviceIdType.MESH
ROWS = (8, 8, 4, 4, 2, 2)
CHANS = (64, 64, 128, 128, 256, 256)


def iota(shape, axis):
    return lax.broadcasted_iota(jnp.int32, shape, axis)


def make_kernel(count):
    def kernel(*refs):
        inputs, (o_ref, *refs) = refs[:ARGS], refs[ARGS:]
        local, refs = refs[:ARGS], refs[ARGS:]
        body(inputs, local, o_ref, *refs)

    def body(inputs, local, o_ref, load_sem,
               slab, recv, zin, t1, tr1, td2, tr2, aff, gmat, smat, pmat, lanes,
               acc, zd1, zr1, zd2, zr2, zd3, fst, outb,
               send_in, recv_in, send_out, recv_out, local_out):
        x_ref, w1d, v1d, w1r, v1r, w2d, v2d, w2r, v2r, w3d, v3d, w3r, v3r = local
        loads = [pltpu.make_async_copy(inputs[n], local[n], load_sem.at[n]) for n in range(ARGS)]
        for load in loads:
            load.start()
        wi = lax.axis_index("w")
        hi = lax.axis_index("h")
        me = hi * 4 + wi
        barrier = pltpu.get_barrier_semaphore()

        def peer(k):
            d = lax.rem(me + k, 16)
            return d, {"h": d // 4, "w": lax.rem(d, 4)}

        for k in range(1, 16):
            pl.semaphore_signal(barrier, inc=1, device_id=peer(k)[1], device_id_type=MESH)

        side = wi // 2
        twin = 2 * hi + lax.rem(wi, 2)

        def first_image(p, h, w):
            solo = 2 * SOLO * (4 * h + w) + 2 * p
            shared = 2 * SOLO * 16 + 2 * (PAIRS - SOLO) * (2 * h + lax.rem(w, 2)) + 2 * (p - SOLO)
            return jnp.where(p < SOLO, solo, shared) if not isinstance(p, int) else (solo if p < SOLO else shared)

        r, c = iota((32, BLOCK), 0), iota((32, BLOCK), 1)
        pmat[...] = ((c // 16 == r % 16) & ((c // 2) % 2 == r // 16)).astype(F32).astype(BF)
        r, c = iota((LANE, BLOCK), 0) // 16, iota((LANE, BLOCK), 1)
        lanes[...] = (((c // 4) % 4 == r // 2) & (c % 2 == r % 2)).astype(F32).astype(BF)

        def pack(ch):
            def step(t, carry):
                wide = []
                for k in (2 * t, 2 * t + 1):
                    dev = peer(k)[1]
                    at = pl.multiple_of(8 * first_image(ch, dev["h"], dev["w"]), 16)
                    wide.append(jnp.concatenate([x_ref[pl.ds(at, 16), :]] * 8, axis=0) * lanes[...])
                turned = lax.dot_general(pmat[...], jnp.concatenate(wide, axis=0), (((1,), (1,)), ((), ())),
                                         preferred_element_type=F32).astype(BF)
                slab[2 * t, ch] = turned[:, :LANE]
                slab[2 * t + 1, ch] = turned[:, LANE:]
                return carry
            lax.fori_loop(0, 8, step, 0)

        def send(g):
            at, size = GROUPS[g]

            def step(k, carry):
                pltpu.make_async_remote_copy(
                    src_ref=slab.at[k, at:at + size], dst_ref=recv.at[me, at:at + size], send_sem=send_in,
                    recv_sem=recv_in.at[g], device_id=peer(k)[1], device_id_type=MESH).start()
                return carry
            lax.fori_loop(1, 16, step, 0)
            recv[me, at:at + size] = slab[0, at:at + size]

        loads[0].wait()
        pack(0)
        pl.semaphore_wait(barrier, 15)
        send(0)
        pack(1)
        pack(2)
        send(1)

        for load in loads[1:]:
            load.wait()
        r, c = iota((512, WIDE), 0), iota((512, WIDE), 1)
        column = (r // LANE == (c // 8) % 4) & (r % 8 == c % 8) & ((r // 32) % 4 == c // BLOCK)
        here = (c % BLOCK < LANE) & ((c // 64) % 2 == (r // 8) % 2) & ((c // 32) % 2 == (r // 16) % 2)
        above = (c % BLOCK >= LANE) & (c % LANE < 64) & ((c // 32) % 2 == (r // 8) % 2) & ((r // 16) % 2 == 1)
        smat[...] = (column & (here | above)).astype(F32).astype(BF)
        r, c = iota((384, LANE), 0) % LANE, iota((384, LANE), 1)
        for s, chan in enumerate((64, LANE, BLOCK)):
            size = chan // 8
            gmat[s] = ((r % chan) // size == (c % chan) // size).astype(F32).astype(BF)
        for s, v in enumerate((v1d, v1r, v2d, v2r, v3d, v3r)):
            chan = CHANS[s]
            if chan == 64:
                aff[s, 0:3, :] = jnp.concatenate([v[...], v[...]], axis=1)
            else:
                aff[s, 0:3, :] = v[:, 0:LANE]
                if chan == BLOCK:
                    aff[s, 3:6, :] = v[:, LANE:BLOCK]
        t1[...] = jnp.zeros_like(t1)
        row, col = iota((32, WIDE), 0), iota((32, WIDE), 1) // 64
        for dh in range(3):
            base = jnp.zeros((32, WIDE), F32)
            for dw in range(3):
                tap = w1d[dh, dw:dw + 1, :].astype(F32)
                tap = jnp.concatenate([tap, tap], axis=1)
                tap = jnp.concatenate([tap] * 8, axis=1)
                base = jnp.where(row == 2 * col + dw - 1, jnp.broadcast_to(tap, (32, WIDE)), base)
            for i in range(2):
                at = LANE + 32 * i if dh == 0 else 64 * i + 32 * (dh - 1)
                t1[i, at:at + 32, :] = base.astype(BF)
        tr1[...] = jnp.zeros_like(tr1)
        td2[...] = jnp.zeros_like(td2)
        tr2[...] = jnp.zeros_like(tr2)
        for dh in range(3):
            for dw in range(3):
                tap = w1r[dh, 64 * dw:64 * dw + 64, :]
                for jo in range(4):
                    ji = jo + 1 + dw
                    tr1[dh, 64 * ji:64 * ji + 64, 64 * jo:64 * jo + 64] = tap
                tap = w2d[dh, 64 * dw:64 * dw + 64, :]
                for jo in range(2):
                    ji = 2 * jo + 1 + dw
                    td2[dh, 64 * ji:64 * ji + 64, LANE * jo:LANE * jo + LANE] = tap
                tap = w2r[dh, LANE * dw:LANE * dw + LANE, :]
                for jo in range(2):
                    ji = jo + dw
                    tr2[dh, LANE * ji:LANE * ji + LANE, LANE * jo:LANE * jo + LANE] = tap

        for ch in range(3, PAIRS):
            pack(ch)
        send(2)

        top = iota((64, BLOCK), 0) == 0
        bottom = iota((64, BLOCK), 0) == 63

        def taps(ref, j, rows, stride, lo, hi_, h0, h1):
            pieces = []
            for dh in range(3):
                if stride == 1:
                    piece = ref[j, h0:h1, dh:dh + rows, :, lo:hi_]
                    pieces.append(piece.reshape((h1 - h0) * 16 * rows, hi_ - lo))
                else:
                    pieces.append(jnp.concatenate(
                        [ref[j, h, 2 * l + dh, :, lo:hi_] for h in range(h0, h1) for l in range(rows)], axis=0))
            return jnp.concatenate(pieces, axis=1)

        def conv(j, s, b, i):
            rows = ROWS[s]
            lo = BLOCK * b
            step = min(4, CHUNK // (16 * rows))
            sums = sqs = None
            for h0 in range(0, 4, step):
                h1 = h0 + step
                m = 16 * rows * step
                if s == 0:
                    lhs = zin[h0:h1, 0:8].reshape(m, BLOCK)
                    rhs = t1[i, :, lo:lo + BLOCK]
                elif s in (1, 3):
                    ref, mat = ((zd1, tr1), (zd2, tr2))[s // 2]
                    first, last = (LANE if b == 0 else 0), (384 if b == 3 else 512)
                    lhs = taps(ref, j, rows, 1, lo - LANE + first, lo - LANE + last, h0, h1)
                    rhs = mat[:, first:last, :].reshape(3 * (last - first), BLOCK)
                elif s in (2, 4):
                    ref, mat = ((zr1, td2), (zr2, w3d))[s // 2 - 1]
                    first = LANE if b == 0 else 0
                    lhs = taps(ref, j, rows, 2, lo - LANE + first, lo + BLOCK, h0, h1)
                    rhs = mat[:, first:384, :].reshape(3 * (384 - first), BLOCK)
                else:
                    first, last = (BLOCK if b == 0 else 0), (512 if b == 3 else 768)
                    lhs = taps(zd3, j, rows, 1, lo - BLOCK + first, lo - BLOCK + last, h0, h1)
                    rhs = w3r[:, first:last, :].reshape(3 * (last - first), BLOCK)
                out = jnp.dot(lhs, rhs, preferred_element_type=F32)
                at = 16 * rows * h0
                acc[j, at:at + m, lo:lo + BLOCK] = out
                tall = out.reshape(m // 8, 8, BLOCK)
                one, two = jnp.sum(tall, axis=0), jnp.sum(tall * tall, axis=0)
                sums, sqs = (one, two) if sums is None else (sums + one, sqs + two)
            return sums, sqs

        def finish(s, parts):
            m, chan = 64 * ROWS[s], CHANS[s]
            sums = parts[0][0] + parts[1][0] + parts[2][0] + parts[3][0]
            sqs = parts[0][1] + parts[1][1] + parts[2][1] + parts[3][1]
            if chan == BLOCK:
                sides, per_lane = [(sums[:, 0:LANE], sqs[:, 0:LANE]), (sums[:, LANE:], sqs[:, LANE:])], 4.0 * m
            else:
                sides, per_lane = [(sums[:, 0:LANE] + sums[:, LANE:], sqs[:, 0:LANE] + sqs[:, LANE:])], 8.0 * m
            count = float(m * WIDE // 8)
            row16 = iota((16, LANE), 0)
            packed = jnp.zeros((16, LANE), F32)
            for n, (one, two) in enumerate(sides):
                bias = aff[s, 3 * n:3 * n + 1, :]
                one = jnp.sum(one, axis=0, keepdims=True)
                two = jnp.sum(two, axis=0, keepdims=True)
                total = one + per_lane * bias
                square = two + bias * (one + total)
                packed = jnp.where(row16 == 2 * n, total, jnp.where(row16 == 2 * n + 1, square, packed))
            high = packed.astype(BF)
            rest = packed - high.astype(F32)
            mid = rest.astype(BF)
            low = (rest - mid.astype(F32)).astype(BF)
            totals = jnp.dot(jnp.concatenate([high, mid, low], axis=1), gmat[s // 2], preferred_element_type=F32)
            scales, shifts = [], []
            for n in range(len(sides)):
                bias, gain, beta = (aff[s, 3 * n + t:3 * n + t + 1, :] for t in range(3))
                mean = totals[2 * n:2 * n + 1] * (1.0 / count)
                var = jnp.maximum(totals[2 * n + 1:2 * n + 2] * (1.0 / count) - mean * mean, 0.0)
                scale = lax.rsqrt(var + NORM_EPS) * gain
                scales.append(scale)
                shifts.append(beta + (bias - mean) * scale)
            if len(sides) == 1:
                scales, shifts = scales * 2, shifts * 2
            return jnp.concatenate(scales, axis=1), jnp.concatenate(shifts, axis=1)

        def norm(j, s, b, affine):
            rows = ROWS[s]
            m = 64 * rows
            lo = BLOCK * b
            z = jnp.maximum(acc[j, 0:m, lo:lo + BLOCK] * affine[0] + affine[1], 0.0).reshape(4, rows, 16, BLOCK)
            if s == 5:
                for h in range(4):
                    for l in range(2):
                        for t in range(2):
                            fst[j, 2 * (4 * h + b) + t, pl.ds(l, 16, stride=2), :] = z[h, l, :, LANE * t:LANE * t + LANE]
                return
            ref = (zd1, zr1, zd2, zr2, zd3)[s]
            ref[j, :, 1:1 + rows, :, lo:lo + BLOCK] = z.astype(BF)
            edge = pltpu.roll(z[:, rows - 1].reshape(64, BLOCK), 1, axis=0)
            ref[j, :, 0, :, lo:lo + BLOCK] = jnp.where(top, 0.0, edge).reshape(4, 16, BLOCK).astype(BF)
            if s in (0, 2, 4):
                edge = pltpu.roll(z[:, 0].reshape(64, BLOCK), 63, axis=0)
                ref[j, :, 1 + rows, :, lo:lo + BLOCK] = jnp.where(bottom, 0.0, edge).reshape(4, 16, BLOCK).astype(BF)

        def out_copy(p, d):
            h, w = d // 4, lax.rem(d, 4)
            return pltpu.make_async_remote_copy(
                src_ref=outb.at[d, pl.ds(2 * p, 2)], dst_ref=o_ref.at[pl.ds(first_image(p, hi, wi), 2)],
                send_sem=send_out, recv_sem=recv_out, device_id={"h": h, "w": w}, device_id_type=MESH)

        def emit(j, n):
            for d in range(16):
                outb[d, n] = jnp.concatenate([fst[j, 2 * d], fst[j, 2 * d + 1]], axis=1).astype(BF)

        def pair(p, carry):
            for g, (at, size) in enumerate(GROUPS):
                @pl.when(p == at)
                def _(g=g, size=size):
                    arrived = recv.at[0:15, 0:size]
                    pltpu.make_async_copy(arrived, arrived, recv_in.at[g]).wait()

            wide = jnp.concatenate([
                jnp.concatenate([recv[4 * h + w, p] for h in range(4)], axis=0) for w in range(4)], axis=1)
            spread = jnp.dot(wide, smat[...], preferred_element_type=F32)
            for lq in range(4):
                here, above = (spread[:, LANE * t:LANE * t + LANE].reshape(4, 2, 16, LANE) for t in (2 * lq, 2 * lq + 1))
                zin[:, 2 * lq:2 * lq + 2, :, :LANE] = here.astype(BF)
                zin[:, 2 * lq + 1:2 * lq + 3, :, LANE:] = above.astype(BF)
            edge = pltpu.roll(above[:, 1].reshape(64, LANE), 1, axis=0)
            edge = jnp.where(iota((64, LANE), 0) == 0, 0.0, edge)
            zin[:, 0, :, LANE:] = edge.astype(BF).reshape(4, 16, LANE)

            waiting = None
            for s in range(6):
                for j in range(2):
                    parts = []
                    for b in range(4):
                        parts.append(conv(j, s, b, j))
                        if waiting is not None:
                            norm(*waiting[0:2], b, waiting[2])
                    waiting = (j, s, finish(s, parts))
                    if s == 0 and j == 0:
                        @pl.when(p < PAIRS)
                        def _():
                            aff[0, 7:8, :] = aff[0, 0:1, :]

            @pl.when(p < PAIRS)
            def _():
                emit(0, 2 * p)

            for b in range(4):
                norm(*waiting[0:2], b, waiting[2])
            emit(1, 2 * p + 1)

            @pl.when(p < SOLO)
            def _():
                for k in range(1, 16):
                    out_copy(p, peer(k)[0]).start()

            @pl.when(p >= SOLO)
            def _():
                for k in range(1, 8):
                    t = lax.rem(twin + k, 8)
                    out_copy(p, 4 * (t // 2) + 2 * side + lax.rem(t, 2)).start()

            return carry

        lax.fori_loop(0, PAIRS, pair, 0)

        for at, size, base in ((0, 2 * SOLO, first_image(0, hi, wi)), (2 * SOLO, 2 * (PAIRS - SOLO), first_image(SOLO, hi, wi))):
            own = pltpu.make_async_copy(outb.at[me, at:at + size], o_ref.at[pl.ds(base, size)], local_out)
            own.start()
            own.wait()
        pltpu.make_async_copy(slab.at[0:15], slab.at[0:15], send_in).wait()
        moved = o_ref.at[0:count - 2 * PAIRS]
        pltpu.make_async_copy(moved, moved, send_out).wait()
        pltpu.make_async_copy(moved, moved, recv_out).wait()

    return kernel


def encode(tile, params):
    count = tile.shape[0]
    rows = tile.reshape(count, BLOCK, 8).transpose(0, 2, 1).reshape(count * 8, BLOCK)
    weights = []
    for n, param in enumerate(params):
        if n == 0:
            weights.append(param.reshape(3, 3, 64))
        elif n % 2 == 0:
            weights.append(param.reshape(3, 3 * param.shape[2], param.shape[3]))
        else:
            weights.append(param)
    operands = [rows, *weights]
    return pl.pallas_call(
        make_kernel(count),
        out_shape=jax.ShapeDtypeStruct((count, 32, BLOCK), BF),
        in_specs=[pl.BlockSpec(memory_space=pltpu.HBM)] * ARGS,
        out_specs=pl.BlockSpec(memory_space=pl.ANY),
        scratch_shapes=[pltpu.VMEM(a.shape, a.dtype) for a in operands] + [
            pltpu.SemaphoreType.DMA((ARGS,)),
            pltpu.VMEM((16, PAIRS, 32, LANE), BF),
            pltpu.VMEM((16, PAIRS, 32, LANE), BF),
            pltpu.VMEM((4, 9, 16, BLOCK), BF),
            pltpu.VMEM((2, BLOCK, WIDE), BF),
            pltpu.VMEM((3, 512, BLOCK), BF),
            pltpu.VMEM((3, 384, BLOCK), BF),
            pltpu.VMEM((3, 512, BLOCK), BF),
            pltpu.VMEM((6, 8, LANE), F32),
            pltpu.VMEM((3, 384, LANE), BF),
            pltpu.VMEM((512, WIDE), BF),
            pltpu.VMEM((32, BLOCK), BF),
            pltpu.VMEM((LANE, BLOCK), BF),
            pltpu.VMEM((2, 512, WIDE), F32),
            pltpu.VMEM((2, 4, 10, 16, WIDE), BF),
            pltpu.VMEM((2, 4, 9, 16, WIDE), BF),
            pltpu.VMEM((2, 4, 6, 16, WIDE), BF),
            pltpu.VMEM((2, 4, 5, 16, WIDE), BF),
            pltpu.VMEM((2, 4, 4, 16, WIDE), BF),
            pltpu.VMEM((2, 32, 32, LANE), F32),
            pltpu.VMEM((16, 2 * PAIRS, 32, BLOCK), BF),
            pltpu.SemaphoreType.DMA,
            pltpu.SemaphoreType.DMA((len(GROUPS),)),
            pltpu.SemaphoreType.DMA,
            pltpu.SemaphoreType.DMA,
            pltpu.SemaphoreType.DMA,
        ],
        compiler_params=pltpu.CompilerParams(
            collective_id=0, has_side_effects=True, vmem_limit_bytes=57 * WIDE * WIDE),
        name="encoder",
    )(*operands)


def solution(mesh):
    act_spec = P("batch", "h", "w")

    def local_forward(tile, *params):
        return encode(tile, params)[:, :, None, :]

    return jax.shard_map(local_forward, mesh=mesh, in_specs=(act_spec,) + (P(),) * 12, out_specs=act_spec, check_vma=False)
```

```python
import jax
import jax.numpy as jnp
from jax import lax
from jax.experimental import pallas as pl
from jax.experimental.pallas import tpu as pltpu
from jax.sharding import PartitionSpec as P

NORM_EPS = 1e-5
LANE = 128
BLOCK = 256
WIDE = 1024
CHUNK = 512
PAIRS = 7
SOLO = 5
GROUPS = ((0, 1), (1, 2), (3, 4))
ARGS = 13
BF = jnp.bfloat16
F32 = jnp.float32
MESH = pl.DeviceIdType.MESH
ROWS = (8, 8, 4, 4, 2, 2)
CHANS = (64, 64, 128, 128, 256, 256)


def iota(shape, axis):
    return lax.broadcasted_iota(jnp.int32, shape, axis)


def make_kernel(count):
    def kernel(*refs):
        inputs, (o_ref, *refs) = refs[:ARGS], refs[ARGS:]
        local, refs = refs[:ARGS], refs[ARGS:]
        body(inputs, local, o_ref, *refs)

    def body(inputs, local, o_ref, load_sem,
               slab, recv, zin, t1, tr1, td2, tr2, aff, gmat, smat, pmat, lanes,
               acc, zd1, zr1, zd2, zr2, zd3, fst, outb,
               send_in, recv_in, send_out, recv_out, local_out):
        x_ref, w1d, v1d, w1r, v1r, w2d, v2d, w2r, v2r, w3d, v3d, w3r, v3r = local
        loads = [pltpu.make_async_copy(inputs[n], local[n], load_sem.at[n]) for n in range(ARGS)]
        for load in loads:
            load.start()
        wi = lax.axis_index("w")
        hi = lax.axis_index("h")
        me = hi * 4 + wi
        barrier = pltpu.get_barrier_semaphore()

        def peer(k):
            d = lax.rem(me + k, 16)
            return d, {"h": d // 4, "w": lax.rem(d, 4)}

        for k in range(1, 16):
            pl.semaphore_signal(barrier, inc=1, device_id=peer(k)[1], device_id_type=MESH)

        side = wi // 2
        twin = 2 * hi + lax.rem(wi, 2)

        def first_image(p, h, w):
            solo = 2 * SOLO * (4 * h + w) + 2 * p
            shared = 2 * SOLO * 16 + 2 * (PAIRS - SOLO) * (2 * h + lax.rem(w, 2)) + 2 * (p - SOLO)
            return jnp.where(p < SOLO, solo, shared) if not isinstance(p, int) else (solo if p < SOLO else shared)

        r, c = iota((32, BLOCK), 0), iota((32, BLOCK), 1)
        pmat[...] = ((c // 16 == r % 16) & ((c // 2) % 2 == r // 16)).astype(F32).astype(BF)
        r, c = iota((LANE, BLOCK), 0) // 16, iota((LANE, BLOCK), 1)
        lanes[...] = (((c // 4) % 4 == r // 2) & (c % 2 == r % 2)).astype(F32).astype(BF)

        def pack(ch):
            def step(t, carry):
                wide = []
                for k in (2 * t, 2 * t + 1):
                    dev = peer(k)[1]
                    at = pl.multiple_of(8 * first_image(ch, dev["h"], dev["w"]), 16)
                    wide.append(jnp.concatenate([x_ref[pl.ds(at, 16), :]] * 8, axis=0) * lanes[...])
                turned = lax.dot_general(pmat[...], jnp.concatenate(wide, axis=0), (((1,), (1,)), ((), ())),
                                         preferred_element_type=F32).astype(BF)
                slab[2 * t, ch] = turned[:, :LANE]
                slab[2 * t + 1, ch] = turned[:, LANE:]
                return carry
            lax.fori_loop(0, 8, step, 0)

        def send(g):
            at, size = GROUPS[g]

            def step(k, carry):
                pltpu.make_async_remote_copy(
                    src_ref=slab.at[k, at:at + size], dst_ref=recv.at[me, at:at + size], send_sem=send_in,
                    recv_sem=recv_in.at[g], device_id=peer(k)[1], device_id_type=MESH).start()
                return carry
            lax.fori_loop(1, 16, step, 0)
            recv[me, at:at + size] = slab[0, at:at + size]

        loads[0].wait()
        pack(0)
        pl.semaphore_wait(barrier, 15)
        send(0)
        pack(1)
        pack(2)
        send(1)

        for load in loads[1:]:
            load.wait()
        r, c = iota((512, WIDE), 0), iota((512, WIDE), 1)
        column = (r // LANE == (c // 8) % 4) & (r % 8 == c % 8) & ((r // 32) % 4 == c // BLOCK)
        here = (c % BLOCK < LANE) & ((c // 64) % 2 == (r // 8) % 2) & ((c // 32) % 2 == (r // 16) % 2)
        above = (c % BLOCK >= LANE) & (c % LANE < 64) & ((c // 32) % 2 == (r // 8) % 2) & ((r // 16) % 2 == 1)
        smat[...] = (column & (here | above)).astype(F32).astype(BF)
        r, c = iota((384, LANE), 0) % LANE, iota((384, LANE), 1)
        for s, chan in enumerate((64, LANE, BLOCK)):
            size = chan // 8
            gmat[s] = ((r % chan) // size == (c % chan) // size).astype(F32).astype(BF)
        for s, v in enumerate((v1d, v1r, v2d, v2r, v3d, v3r)):
            chan = CHANS[s]
            if chan == 64:
                aff[s, 0:3, :] = jnp.concatenate([v[...], v[...]], axis=1)
            else:
                aff[s, 0:3, :] = v[:, 0:LANE]
                if chan == BLOCK:
                    aff[s, 3:6, :] = v[:, LANE:BLOCK]
        t1[...] = jnp.zeros_like(t1)
        row, col = iota((32, WIDE), 0), iota((32, WIDE), 1) // 64
        for dh in range(3):
            base = jnp.zeros((32, WIDE), F32)
            for dw in range(3):
                tap = w1d[dh, dw:dw + 1, :].astype(F32)
                tap = jnp.concatenate([tap, tap], axis=1)
                tap = jnp.concatenate([tap] * 8, axis=1)
                base = jnp.where(row == 2 * col + dw - 1, jnp.broadcast_to(tap, (32, WIDE)), base)
            for i in range(2):
                at = LANE + 32 * i if dh == 0 else 64 * i + 32 * (dh - 1)
                t1[i, at:at + 32, :] = base.astype(BF)
        tr1[...] = jnp.zeros_like(tr1)
        td2[...] = jnp.zeros_like(td2)
        tr2[...] = jnp.zeros_like(tr2)
        for dh in range(3):
            for dw in range(3):
                tap = w1r[dh, 64 * dw:64 * dw + 64, :]
                for jo in range(4):
                    ji = jo + 1 + dw
                    tr1[dh, 64 * ji:64 * ji + 64, 64 * jo:64 * jo + 64] = tap
                tap = w2d[dh, 64 * dw:64 * dw + 64, :]
                for jo in range(2):
                    ji = 2 * jo + 1 + dw
                    td2[dh, 64 * ji:64 * ji + 64, LANE * jo:LANE * jo + LANE] = tap
                tap = w2r[dh, LANE * dw:LANE * dw + LANE, :]
                for jo in range(2):
                    ji = jo + dw
                    tr2[dh, LANE * ji:LANE * ji + LANE, LANE * jo:LANE * jo + LANE] = tap

        for ch in range(3, PAIRS):
            pack(ch)
        send(2)

        top = iota((64, BLOCK), 0) == 0
        bottom = iota((64, BLOCK), 0) == 63

        def taps(ref, j, rows, stride, lo, hi_, h0, h1):
            pieces = []
            for dh in range(3):
                if stride == 1:
                    piece = ref[j, h0:h1, dh:dh + rows, :, lo:hi_]
                    pieces.append(piece.reshape((h1 - h0) * 16 * rows, hi_ - lo))
                else:
                    pieces.append(jnp.concatenate(
                        [ref[j, h, 2 * l + dh, :, lo:hi_] for h in range(h0, h1) for l in range(rows)], axis=0))
            return jnp.concatenate(pieces, axis=1)

        def conv(j, s, b, i):
            rows = ROWS[s]
            lo = BLOCK * b
            step = min(4, CHUNK // (16 * rows))
            sums = sqs = None
            for h0 in range(0, 4, step):
                h1 = h0 + step
                m = 16 * rows * step
                if s == 0:
                    lhs = zin[h0:h1, 0:8].reshape(m, BLOCK)
                    rhs = t1[i, :, lo:lo + BLOCK]
                elif s in (1, 3):
                    ref, mat = ((zd1, tr1), (zd2, tr2))[s // 2]
                    first, last = (LANE if b == 0 else 0), (384 if b == 3 else 512)
                    lhs = taps(ref, j, rows, 1, lo - LANE + first, lo - LANE + last, h0, h1)
                    rhs = mat[:, first:last, :].reshape(3 * (last - first), BLOCK)
                elif s in (2, 4):
                    ref, mat = ((zr1, td2), (zr2, w3d))[s // 2 - 1]
                    first = LANE if b == 0 else 0
                    lhs = taps(ref, j, rows, 2, lo - LANE + first, lo + BLOCK, h0, h1)
                    rhs = mat[:, first:384, :].reshape(3 * (384 - first), BLOCK)
                else:
                    first, last = (BLOCK if b == 0 else 0), (512 if b == 3 else 768)
                    lhs = taps(zd3, j, rows, 1, lo - BLOCK + first, lo - BLOCK + last, h0, h1)
                    rhs = w3r[:, first:last, :].reshape(3 * (last - first), BLOCK)
                out = jnp.dot(lhs, rhs, preferred_element_type=F32)
                at = 16 * rows * h0
                acc[j, at:at + m, lo:lo + BLOCK] = out
                tall = out.reshape(m // 8, 8, BLOCK)
                one, two = jnp.sum(tall, axis=0), jnp.sum(tall * tall, axis=0)
                sums, sqs = (one, two) if sums is None else (sums + one, sqs + two)
            return sums, sqs

        def finish(s, parts):
            m, chan = 64 * ROWS[s], CHANS[s]
            sums = parts[0][0] + parts[1][0] + parts[2][0] + parts[3][0]
            sqs = parts[0][1] + parts[1][1] + parts[2][1] + parts[3][1]
            if chan == BLOCK:
                sides, per_lane = [(sums[:, 0:LANE], sqs[:, 0:LANE]), (sums[:, LANE:], sqs[:, LANE:])], 4.0 * m
            else:
                sides, per_lane = [(sums[:, 0:LANE] + sums[:, LANE:], sqs[:, 0:LANE] + sqs[:, LANE:])], 8.0 * m
            count = float(m * WIDE // 8)
            row16 = iota((16, LANE), 0)
            packed = jnp.zeros((16, LANE), F32)
            for n, (one, two) in enumerate(sides):
                bias = aff[s, 3 * n:3 * n + 1, :]
                one = jnp.sum(one, axis=0, keepdims=True)
                two = jnp.sum(two, axis=0, keepdims=True)
                total = one + per_lane * bias
                square = two + bias * (one + total)
                packed = jnp.where(row16 == 2 * n, total, jnp.where(row16 == 2 * n + 1, square, packed))
            high = packed.astype(BF)
            rest = packed - high.astype(F32)
            mid = rest.astype(BF)
            low = (rest - mid.astype(F32)).astype(BF)
            totals = jnp.dot(jnp.concatenate([high, mid, low], axis=1), gmat[s // 2], preferred_element_type=F32)
            scales, shifts = [], []
            for n in range(len(sides)):
                bias, gain, beta = (aff[s, 3 * n + t:3 * n + t + 1, :] for t in range(3))
                mean = totals[2 * n:2 * n + 1] * (1.0 / count)
                var = jnp.maximum(totals[2 * n + 1:2 * n + 2] * (1.0 / count) - mean * mean, 0.0)
                scale = lax.rsqrt(var + NORM_EPS) * gain
                scales.append(scale)
                shifts.append(beta + (bias - mean) * scale)
            if len(sides) == 1:
                scales, shifts = scales * 2, shifts * 2
            return jnp.concatenate(scales, axis=1), jnp.concatenate(shifts, axis=1)

        def norm(j, s, b, affine):
            rows = ROWS[s]
            m = 64 * rows
            lo = BLOCK * b
            z = jnp.maximum(acc[j, 0:m, lo:lo + BLOCK] * affine[0] + affine[1], 0.0).reshape(4, rows, 16, BLOCK)
            if s == 5:
                for h in range(4):
                    for l in range(2):
                        for t in range(2):
                            fst[j, 2 * (4 * h + b) + t, pl.ds(l, 16, stride=2), :] = z[h, l, :, LANE * t:LANE * t + LANE]
                return
            ref = (zd1, zr1, zd2, zr2, zd3)[s]
            ref[j, :, 1:1 + rows, :, lo:lo + BLOCK] = z.astype(BF)
            edge = pltpu.roll(z[:, rows - 1].reshape(64, BLOCK), 1, axis=0)
            ref[j, :, 0, :, lo:lo + BLOCK] = jnp.where(top, 0.0, edge).reshape(4, 16, BLOCK).astype(BF)
            if s in (0, 2, 4):
                edge = pltpu.roll(z[:, 0].reshape(64, BLOCK), 63, axis=0)
                ref[j, :, 1 + rows, :, lo:lo + BLOCK] = jnp.where(bottom, 0.0, edge).reshape(4, 16, BLOCK).astype(BF)

        def out_copy(p, d):
            h, w = d // 4, lax.rem(d, 4)
            return pltpu.make_async_remote_copy(
                src_ref=outb.at[d, pl.ds(2 * p, 2)], dst_ref=o_ref.at[pl.ds(first_image(p, hi, wi), 2)],
                send_sem=send_out, recv_sem=recv_out, device_id={"h": h, "w": w}, device_id_type=MESH)

        def emit(j, n):
            for d in range(16):
                outb[d, n] = jnp.concatenate([fst[j, 2 * d], fst[j, 2 * d + 1]], axis=1).astype(BF)

        def pair(p, carry):
            for g, (at, size) in enumerate(GROUPS):
                @pl.when(p == at)
                def _(g=g, size=size):
                    arrived = recv.at[0:15, 0:size]
                    pltpu.make_async_copy(arrived, arrived, recv_in.at[g]).wait()

            wide = jnp.concatenate([
                jnp.concatenate([recv[4 * h + w, p] for h in range(4)], axis=0) for w in range(4)], axis=1)
            spread = jnp.dot(wide, smat[...], preferred_element_type=F32)
            for lq in range(4):
                here, above = (spread[:, LANE * t:LANE * t + LANE].reshape(4, 2, 16, LANE) for t in (2 * lq, 2 * lq + 1))
                zin[:, 2 * lq:2 * lq + 2, :, :LANE] = here.astype(BF)
                zin[:, 2 * lq + 1:2 * lq + 3, :, LANE:] = above.astype(BF)
            edge = pltpu.roll(above[:, 1].reshape(64, LANE), 1, axis=0)
            edge = jnp.where(iota((64, LANE), 0) == 0, 0.0, edge)
            zin[:, 0, :, LANE:] = edge.astype(BF).reshape(4, 16, LANE)

            waiting = None
            for s in range(6):
                for j in range(2):
                    parts = []
                    for b in range(4):
                        parts.append(conv(j, s, b, j))
                        if waiting is not None:
                            if b == 0:
                                affine = finish(waiting[1], waiting[2])
                            else:
                                norm(*waiting[0:2], b - 1, affine)
                            if b == 3:
                                norm(*waiting[0:2], b, affine)
                    waiting = (j, s, parts)
                    if s == 0 and j == 0:
                        @pl.when(p < PAIRS)
                        def _():
                            aff[0, 7:8, :] = aff[0, 0:1, :]

            @pl.when(p < PAIRS)
            def _():
                emit(0, 2 * p)

            affine = finish(waiting[1], waiting[2])
            for b in range(4):
                norm(*waiting[0:2], b, affine)
            emit(1, 2 * p + 1)

            @pl.when(p < SOLO)
            def _():
                for k in range(1, 16):
                    out_copy(p, peer(k)[0]).start()

            @pl.when(p >= SOLO)
            def _():
                for k in range(1, 8):
                    t = lax.rem(twin + k, 8)
                    out_copy(p, 4 * (t // 2) + 2 * side + lax.rem(t, 2)).start()

            return carry

        lax.fori_loop(0, PAIRS, pair, 0)

        for at, size, base in ((0, 2 * SOLO, first_image(0, hi, wi)), (2 * SOLO, 2 * (PAIRS - SOLO), first_image(SOLO, hi, wi))):
            own = pltpu.make_async_copy(outb.at[me, at:at + size], o_ref.at[pl.ds(base, size)], local_out)
            own.start()
            own.wait()
        pltpu.make_async_copy(slab.at[0:15], slab.at[0:15], send_in).wait()
        moved = o_ref.at[0:count - 2 * PAIRS]
        pltpu.make_async_copy(moved, moved, send_out).wait()
        pltpu.make_async_copy(moved, moved, recv_out).wait()

    return kernel


def encode(tile, params):
    count = tile.shape[0]
    rows = tile.reshape(count, BLOCK, 8).transpose(0, 2, 1).reshape(count * 8, BLOCK)
    weights = []
    for n, param in enumerate(params):
        if n == 0:
            weights.append(param.reshape(3, 3, 64))
        elif n % 2 == 0:
            weights.append(param.reshape(3, 3 * param.shape[2], param.shape[3]))
        else:
            weights.append(param)
    operands = [rows, *weights]
    return pl.pallas_call(
        make_kernel(count),
        out_shape=jax.ShapeDtypeStruct((count, 32, BLOCK), BF),
        in_specs=[pl.BlockSpec(memory_space=pltpu.HBM)] * ARGS,
        out_specs=pl.BlockSpec(memory_space=pl.ANY),
        scratch_shapes=[pltpu.VMEM(a.shape, a.dtype) for a in operands] + [
            pltpu.SemaphoreType.DMA((ARGS,)),
            pltpu.VMEM((16, PAIRS, 32, LANE), BF),
            pltpu.VMEM((16, PAIRS, 32, LANE), BF),
            pltpu.VMEM((4, 9, 16, BLOCK), BF),
            pltpu.VMEM((2, BLOCK, WIDE), BF),
            pltpu.VMEM((3, 512, BLOCK), BF),
            pltpu.VMEM((3, 384, BLOCK), BF),
            pltpu.VMEM((3, 512, BLOCK), BF),
            pltpu.VMEM((6, 8, LANE), F32),
            pltpu.VMEM((3, 384, LANE), BF),
            pltpu.VMEM((512, WIDE), BF),
            pltpu.VMEM((32, BLOCK), BF),
            pltpu.VMEM((LANE, BLOCK), BF),
            pltpu.VMEM((2, 512, WIDE), F32),
            pltpu.VMEM((2, 4, 10, 16, WIDE), BF),
            pltpu.VMEM((2, 4, 9, 16, WIDE), BF),
            pltpu.VMEM((2, 4, 6, 16, WIDE), BF),
            pltpu.VMEM((2, 4, 5, 16, WIDE), BF),
            pltpu.VMEM((2, 4, 4, 16, WIDE), BF),
            pltpu.VMEM((2, 32, 32, LANE), F32),
            pltpu.VMEM((16, 2 * PAIRS, 32, BLOCK), BF),
            pltpu.SemaphoreType.DMA,
            pltpu.SemaphoreType.DMA((len(GROUPS),)),
            pltpu.SemaphoreType.DMA,
            pltpu.SemaphoreType.DMA,
            pltpu.SemaphoreType.DMA,
        ],
        compiler_params=pltpu.CompilerParams(
            collective_id=0, has_side_effects=True, vmem_limit_bytes=57 * WIDE * WIDE),
        name="encoder",
    )(*operands)


def solution(mesh):
    act_spec = P("batch", "h", "w")

    def local_forward(tile, *params):
        return encode(tile, params)[:, :, None, :]

    return jax.shard_map(local_forward, mesh=mesh, in_specs=(act_spec,) + (P(),) * 12, out_specs=act_spec, check_vma=False)
```

```python
import jax
import jax.numpy as jnp
from jax import lax
from jax.experimental import pallas as pl
from jax.experimental.pallas import tpu as pltpu
from jax.sharding import PartitionSpec as P

NORM_EPS = 1e-5
SPAN = 512
LANE = 128
BLOCK = 256
WIDE = 1024
CHUNK = 512
PAIRS = 7
SOLO = 5
GROUPS = ((0, 1), (1, 2), (3, 4))
ARGS = 13
STEPS = 8
BF = jnp.bfloat16
F32 = jnp.float32
MESH = pl.DeviceIdType.MESH
ROWS = (8, 8, 4, 4, 2, 2)
CHANS = (64, 64, 128, 128, 256, 256)


def iota(shape, axis):
    return lax.broadcasted_iota(jnp.int32, shape, axis)


def make_kernel(count):
    def kernel(*refs):
        inputs, (o_ref, *refs) = refs[:ARGS], refs[ARGS:]
        local, refs = refs[:ARGS], refs[ARGS:]
        body(inputs, local, o_ref, *refs)

    def body(inputs, local, o_ref, load_sem,
               slab, recv, zin, t1, tr1, td2, tr2, aff, gmat, smat, pmat, lanes,
               acc, zd1, zr1, zd2, zr2, zd3, fst, outb,
               send_in, recv_in, send_out, recv_out, local_out):
        x_ref, w1d, v1d, w1r, v1r, w2d, v2d, w2r, v2r, w3d, v3d, w3r, v3r = local
        loads = [pltpu.make_async_copy(inputs[n], local[n], load_sem.at[n]) for n in range(ARGS)]
        for load in loads:
            load.start()
        wi = lax.axis_index("w")
        hi = lax.axis_index("h")
        me = hi * 4 + wi
        barrier = pltpu.get_barrier_semaphore()

        def peer(k):
            d = lax.rem(me + k, 16)
            return d, {"h": d // 4, "w": lax.rem(d, 4)}

        for k in range(1, 16):
            pl.semaphore_signal(barrier, inc=1, device_id=peer(k)[1], device_id_type=MESH)

        side = wi // 2
        twin = 2 * hi + lax.rem(wi, 2)

        def first_image(p, h, w):
            solo = 2 * SOLO * (4 * h + w) + 2 * p
            shared = 2 * SOLO * 16 + 2 * (PAIRS - SOLO) * (2 * h + lax.rem(w, 2)) + 2 * (p - SOLO)
            return jnp.where(p < SOLO, solo, shared) if not isinstance(p, int) else (solo if p < SOLO else shared)

        r, c = iota((32, BLOCK), 0), iota((32, BLOCK), 1)
        pmat[...] = ((c // 16 == r % 16) & ((c // 2) % 2 == r // 16)).astype(F32).astype(BF)
        r, c = iota((LANE, BLOCK), 0) // 16, iota((LANE, BLOCK), 1)
        lanes[...] = (((c // 4) % 4 == r // 2) & (c % 2 == r % 2)).astype(F32).astype(BF)

        def pack(ch):
            def step(t, carry):
                wide = []
                for k in (2 * t, 2 * t + 1):
                    dev = peer(k)[1]
                    at = pl.multiple_of(8 * first_image(ch, dev["h"], dev["w"]), 16)
                    wide.append(jnp.concatenate([x_ref[pl.ds(at, 16), :]] * 8, axis=0) * lanes[...])
                turned = lax.dot_general(pmat[...], jnp.concatenate(wide, axis=0), (((1,), (1,)), ((), ())),
                                         preferred_element_type=F32).astype(BF)
                slab[2 * t, ch] = turned[:, :LANE]
                slab[2 * t + 1, ch] = turned[:, LANE:]
                return carry
            lax.fori_loop(0, 8, step, 0)

        def send(g):
            at, size = GROUPS[g]

            def step(k, carry):
                pltpu.make_async_remote_copy(
                    src_ref=slab.at[k, at:at + size], dst_ref=recv.at[me, at:at + size], send_sem=send_in,
                    recv_sem=recv_in.at[g], device_id=peer(k)[1], device_id_type=MESH).start()
                return carry
            lax.fori_loop(1, 16, step, 0)
            recv[me, at:at + size] = slab[0, at:at + size]

        loads[0].wait()
        pack(0)
        pl.semaphore_wait(barrier, 15)
        send(0)
        pack(1)
        pack(2)
        send(1)

        for load in loads[1:]:
            load.wait()
        r, c = iota((SPAN, WIDE), 0), iota((SPAN, WIDE), 1)
        column = (r // LANE == (c // 8) % 4) & (r % 8 == c % 8) & ((r // 32) % 4 == c // BLOCK)
        here = (c % BLOCK < LANE) & ((c // 64) % 2 == (r // 8) % 2) & ((c // 32) % 2 == (r // 16) % 2)
        above = (c % BLOCK >= LANE) & (c % LANE < 64) & ((c // 32) % 2 == (r // 8) % 2) & ((r // 16) % 2 == 1)
        smat[...] = (column & (here | above)).astype(F32).astype(BF)
        r, c = iota((384, LANE), 0) % LANE, iota((384, LANE), 1)
        for s, chan in enumerate((64, LANE, BLOCK)):
            size = chan // 8
            gmat[s] = ((r % chan) // size == (c % chan) // size).astype(F32).astype(BF)
        for s, v in enumerate((v1d, v1r, v2d, v2r, v3d, v3r)):
            chan = CHANS[s]
            if chan == 64:
                aff[s, 0:3, :] = jnp.concatenate([v[...], v[...]], axis=1)
            else:
                aff[s, 0:3, :] = v[:, 0:LANE]
                if chan == BLOCK:
                    aff[s, 3:6, :] = v[:, LANE:BLOCK]
        t1[...] = jnp.zeros_like(t1)
        row, col = iota((32, WIDE), 0), iota((32, WIDE), 1) // 64
        for dh in range(3):
            base = jnp.zeros((32, WIDE), F32)
            for dw in range(3):
                tap = w1d[dh, dw:dw + 1, :].astype(F32)
                tap = jnp.concatenate([tap, tap], axis=1)
                tap = jnp.concatenate([tap] * 8, axis=1)
                base = jnp.where(row == 2 * col + dw - 1, jnp.broadcast_to(tap, (32, WIDE)), base)
            for i in range(2):
                at = LANE + 32 * i if dh == 0 else 64 * i + 32 * (dh - 1)
                t1[i, at:at + 32, :] = base.astype(BF)
        tr1[...] = jnp.zeros_like(tr1)
        td2[...] = jnp.zeros_like(td2)
        tr2[...] = jnp.zeros_like(tr2)
        for dh in range(3):
            for dw in range(3):
                tap = w1r[dh, 64 * dw:64 * dw + 64, :]
                for jo in range(4):
                    ji = jo + 1 + dw
                    tr1[dh, 64 * ji:64 * ji + 64, 64 * jo:64 * jo + 64] = tap
                tap = w2d[dh, 64 * dw:64 * dw + 64, :]
                for jo in range(2):
                    ji = 2 * jo + 1 + dw
                    td2[dh, 64 * ji:64 * ji + 64, LANE * jo:LANE * jo + LANE] = tap
                tap = w2r[dh, LANE * dw:LANE * dw + LANE, :]
                for jo in range(2):
                    ji = jo + dw
                    tr2[dh, LANE * ji:LANE * ji + LANE, LANE * jo:LANE * jo + LANE] = tap

        for ch in range(3, PAIRS):
            pack(ch)
        send(2)

        top = iota((64, BLOCK), 0) == 0
        bottom = iota((64, BLOCK), 0) == 63

        def taps(ref, j, rows, stride, lo, hi_, h0, h1):
            pieces = []
            for dh in range(3):
                if stride == 1:
                    piece = ref[j, h0:h1, dh:dh + rows, :, lo:hi_]
                    pieces.append(piece.reshape((h1 - h0) * 16 * rows, hi_ - lo))
                else:
                    pieces.append(jnp.concatenate(
                        [ref[j, h, 2 * l + dh, :, lo:hi_] for h in range(h0, h1) for l in range(rows)], axis=0))
            return jnp.concatenate(pieces, axis=1)

        def conv(j, s, b, i):
            rows = ROWS[s]
            lo = BLOCK * b
            step = min(4, CHUNK // (16 * rows))
            sums = sqs = None
            for h0 in range(0, 4, step):
                h1 = h0 + step
                m = 16 * rows * step
                if s == 0:
                    lhs = zin[h0:h1, 0:8].reshape(m, BLOCK)
                    rhs = t1[i, :, lo:lo + BLOCK]
                elif s in (1, 3):
                    ref, mat = ((zd1, tr1), (zd2, tr2))[s // 2]
                    first, last = (LANE if b == 0 else 0), (384 if b == 3 else SPAN)
                    lhs = taps(ref, j, rows, 1, lo - LANE + first, lo - LANE + last, h0, h1)
                    rhs = mat[:, first:last, :].reshape(3 * (last - first), BLOCK)
                elif s in (2, 4):
                    ref, mat = ((zr1, td2), (zr2, w3d))[s // 2 - 1]
                    first = LANE if b == 0 else 0
                    lhs = taps(ref, j, rows, 2, lo - LANE + first, lo + BLOCK, h0, h1)
                    rhs = mat[:, first:384, :].reshape(3 * (384 - first), BLOCK)
                else:
                    first, last = (BLOCK if b == 0 else 0), (SPAN if b == 3 else 768)
                    lhs = taps(zd3, j, rows, 1, lo - BLOCK + first, lo - BLOCK + last, h0, h1)
                    rhs = w3r[:, first:last, :].reshape(3 * (last - first), BLOCK)
                out = jnp.dot(lhs, rhs, preferred_element_type=F32)
                at = 16 * rows * h0
                acc[j, at:at + m, lo:lo + BLOCK] = out
                tall = out.reshape(m // 8, 8, BLOCK)
                one, two = jnp.sum(tall, axis=0), jnp.sum(tall * tall, axis=0)
                sums, sqs = (one, two) if sums is None else (sums + one, sqs + two)
            return sums, sqs

        def finish(s, parts):
            m, chan = 64 * ROWS[s], CHANS[s]
            sums = parts[0][0] + parts[1][0] + parts[2][0] + parts[3][0]
            sqs = parts[0][1] + parts[1][1] + parts[2][1] + parts[3][1]
            if chan == BLOCK:
                sides, per_lane = [(sums[:, 0:LANE], sqs[:, 0:LANE]), (sums[:, LANE:], sqs[:, LANE:])], 4.0 * m
            else:
                sides, per_lane = [(sums[:, 0:LANE] + sums[:, LANE:], sqs[:, 0:LANE] + sqs[:, LANE:])], 8.0 * m
            count = float(m * WIDE // 8)
            row16 = iota((16, LANE), 0)
            packed = jnp.zeros((16, LANE), F32)
            for n, (one, two) in enumerate(sides):
                bias = aff[s, 3 * n:3 * n + 1, :]
                one = jnp.sum(one, axis=0, keepdims=True)
                two = jnp.sum(two, axis=0, keepdims=True)
                total = one + per_lane * bias
                square = two + bias * (one + total)
                packed = jnp.where(row16 == 2 * n, total, jnp.where(row16 == 2 * n + 1, square, packed))
            high = packed.astype(BF)
            rest = packed - high.astype(F32)
            mid = rest.astype(BF)
            low = (rest - mid.astype(F32)).astype(BF)
            totals = jnp.dot(jnp.concatenate([high, mid, low], axis=1), gmat[s // 2], preferred_element_type=F32)
            scales, shifts = [], []
            for n in range(len(sides)):
                bias, gain, beta = (aff[s, 3 * n + t:3 * n + t + 1, :] for t in range(3))
                mean = totals[2 * n:2 * n + 1] * (1.0 / count)
                var = jnp.maximum(totals[2 * n + 1:2 * n + 2] * (1.0 / count) - mean * mean, 0.0)
                scale = lax.rsqrt(var + NORM_EPS) * gain
                scales.append(scale)
                shifts.append(beta + (bias - mean) * scale)
            if len(sides) == 1:
                scales, shifts = scales * 2, shifts * 2
            return jnp.concatenate(scales, axis=1), jnp.concatenate(shifts, axis=1)

        def norm(j, s, b, affine):
            rows = ROWS[s]
            m = 64 * rows
            lo = BLOCK * b
            z = jnp.maximum(acc[j, 0:m, lo:lo + BLOCK] * affine[0] + affine[1], 0.0).reshape(4, rows, 16, BLOCK)
            if s == 5:
                for h in range(4):
                    for l in range(2):
                        for t in range(2):
                            fst[j, 2 * (4 * h + b) + t, pl.ds(l, 16, stride=2), :] = z[h, l, :, LANE * t:LANE * t + LANE]
                return
            ref = (zd1, zr1, zd2, zr2, zd3)[s]
            ref[j, :, 1:1 + rows, :, lo:lo + BLOCK] = z.astype(BF)
            edge = pltpu.roll(z[:, rows - 1].reshape(64, BLOCK), 1, axis=0)
            ref[j, :, 0, :, lo:lo + BLOCK] = jnp.where(top, 0.0, edge).reshape(4, 16, BLOCK).astype(BF)
            if s in (0, 2, 4):
                edge = pltpu.roll(z[:, 0].reshape(64, BLOCK), 63, axis=0)
                ref[j, :, 1 + rows, :, lo:lo + BLOCK] = jnp.where(bottom, 0.0, edge).reshape(4, 16, BLOCK).astype(BF)

        def out_copy(p, d):
            h, w = d // 4, lax.rem(d, 4)
            return pltpu.make_async_remote_copy(
                src_ref=outb.at[d, pl.ds(2 * p, 2)], dst_ref=o_ref.at[pl.ds(first_image(p, hi, wi), 2)],
                send_sem=send_out, recv_sem=recv_out, device_id={"h": h, "w": w}, device_id_type=MESH)

        def emit(j, n):
            for d in range(16):
                outb[d, n] = jnp.concatenate([fst[j, 2 * d], fst[j, 2 * d + 1]], axis=1).astype(BF)

        def pair(p, carry):
            for g, (at, size) in enumerate(GROUPS):
                @pl.when(p == at)
                def _(g=g, size=size):
                    arrived = recv.at[0:15, 0:size]
                    pltpu.make_async_copy(arrived, arrived, recv_in.at[g]).wait()

            wide = jnp.concatenate([
                jnp.concatenate([recv[4 * h + w, p] for h in range(4)], axis=0) for w in range(4)], axis=1)
            spread = jnp.dot(wide, smat[...], preferred_element_type=F32)
            for lq in range(4):
                here, above = (spread[:, LANE * t:LANE * t + LANE].reshape(4, 2, 16, LANE) for t in (2 * lq, 2 * lq + 1))
                zin[:, 2 * lq:2 * lq + 2, :, :LANE] = here.astype(BF)
                zin[:, 2 * lq + 1:2 * lq + 3, :, LANE:] = above.astype(BF)
            edge = pltpu.roll(above[:, 1].reshape(64, LANE), 1, axis=0)
            edge = jnp.where(iota((64, LANE), 0) == 0, 0.0, edge)
            zin[:, 0, :, LANE:] = edge.astype(BF).reshape(4, 16, LANE)

            waiting = None
            for s in range(6):
                for j in range(2):
                    parts = []
                    for b in range(4):
                        parts.append(conv(j, s, b, j))
                        if waiting is not None:
                            if b == 0:
                                affine = finish(waiting[1], waiting[2])
                            else:
                                norm(*waiting[0:2], b - 1, affine)
                            if b == 3:
                                norm(*waiting[0:2], b, affine)
                    waiting = (j, s, parts)
                    if s == 0 and j == 0:
                        @pl.when(p < PAIRS)
                        def _():
                            aff[0, 7:8, :] = aff[0, 0:1, :]

            @pl.when(p < PAIRS)
            def _():
                emit(0, 2 * p)

            affine = finish(waiting[1], waiting[2])
            for b in range(4):
                norm(*waiting[0:2], b, affine)
            emit(1, 2 * p + 1)

            @pl.when(p < SOLO)
            def _():
                for k in range(1, 16):
                    out_copy(p, peer(k)[0]).start()

            @pl.when(p >= SOLO)
            def _():
                for k in range(1, 8):
                    t = lax.rem(twin + k, 8)
                    out_copy(p, 4 * (t // 2) + 2 * side + lax.rem(t, 2)).start()

            return carry

        lax.fori_loop(0, PAIRS, pair, 0)

        for at, size, base in ((0, 2 * SOLO, first_image(0, hi, wi)), (2 * SOLO, 2 * (PAIRS - SOLO), first_image(SOLO, hi, wi))):
            own = pltpu.make_async_copy(outb.at[me, at:at + size], o_ref.at[pl.ds(base, size)], local_out)
            own.start()
            own.wait()
        pltpu.make_async_copy(slab.at[0:15], slab.at[0:15], send_in).wait()
        moved = o_ref.at[0:count - 2 * PAIRS]
        pltpu.make_async_copy(moved, moved, send_out).wait()
        pltpu.make_async_copy(moved, moved, recv_out).wait()

    return kernel


def encode(tile, params):
    count = tile.shape[0]
    rows = tile.reshape(count, BLOCK, 8).transpose(0, 2, 1).reshape(count * 8, BLOCK)
    weights = []
    for n, param in enumerate(params):
        if n == 0:
            weights.append(param.reshape(3, 3, 64))
        elif n % 2 == 0:
            weights.append(param.reshape(3, 3 * param.shape[2], param.shape[3]))
        else:
            weights.append(param)
    operands = [rows, *weights]
    return pl.pallas_call(
        make_kernel(count),
        out_shape=jax.ShapeDtypeStruct((count, 32, BLOCK), BF),
        in_specs=[pl.BlockSpec(memory_space=pltpu.HBM)] * ARGS,
        out_specs=pl.BlockSpec(memory_space=pl.ANY),
        scratch_shapes=[pltpu.VMEM(a.shape, a.dtype) for a in operands] + [
            pltpu.SemaphoreType.DMA((ARGS,)),
            pltpu.VMEM((16, PAIRS, 32, LANE), BF),
            pltpu.VMEM((16, PAIRS, 32, LANE), BF),
            pltpu.VMEM((4, 9, 16, BLOCK), BF),
            pltpu.VMEM((2, BLOCK, WIDE), BF),
            pltpu.VMEM((3, SPAN, BLOCK), BF),
            pltpu.VMEM((3, 384, BLOCK), BF),
            pltpu.VMEM((3, SPAN, BLOCK), BF),
            pltpu.VMEM((6, 8, LANE), F32),
            pltpu.VMEM((3, 384, LANE), BF),
            pltpu.VMEM((SPAN, WIDE), BF),
            pltpu.VMEM((32, BLOCK), BF),
            pltpu.VMEM((LANE, BLOCK), BF),
            pltpu.VMEM((2, SPAN, WIDE), F32),
            pltpu.VMEM((2, 4, 10, 16, WIDE), BF),
            pltpu.VMEM((2, 4, 9, 16, WIDE), BF),
            pltpu.VMEM((2, 4, 6, 16, WIDE), BF),
            pltpu.VMEM((2, 4, 5, 16, WIDE), BF),
            pltpu.VMEM((2, 4, 4, 16, WIDE), BF),
            pltpu.VMEM((2, 32, 32, LANE), F32),
            pltpu.VMEM((16, 2 * PAIRS, 32, BLOCK), BF),
            pltpu.SemaphoreType.DMA,
            pltpu.SemaphoreType.DMA((len(GROUPS),)),
            pltpu.SemaphoreType.DMA,
            pltpu.SemaphoreType.DMA,
            pltpu.SemaphoreType.DMA,
        ],
        compiler_params=pltpu.CompilerParams(
            collective_id=0, has_side_effects=True, vmem_limit_bytes=57 * WIDE * WIDE),
        name="encoder",
    )(*operands)


def hand_over(part):
    size = part.shape[0] // STEPS

    def kernel(src, dst, held, load_sem, store_sem):
        loads, stores = ([pltpu.make_async_copy(a.at[size * n:size * n + size], b.at[size * n:size * n + size], c.at[n])
                          for n in range(STEPS)] for a, b, c in ((src, held, load_sem), (held, dst, store_sem)))
        for load in loads:
            load.start()
        for load, store in zip(loads, stores):
            load.wait()
            store.start()
        for store in stores:
            store.wait()

    anywhere = pl.BlockSpec(memory_space=pltpu.HBM)
    return pl.pallas_call(
        kernel, out_shape=jax.ShapeDtypeStruct(part.shape, part.dtype), in_specs=[anywhere], out_specs=anywhere,
        scratch_shapes=[pltpu.VMEM(part.shape, part.dtype), pltpu.SemaphoreType.DMA((STEPS,)), pltpu.SemaphoreType.DMA((STEPS,))],
        compiler_params=pltpu.CompilerParams(vmem_limit_bytes=58 * WIDE * WIDE), name="hand_over")(part)


def solution(mesh):
    act_spec = P("batch", "h", "w")

    def local_forward(tile, *params):
        return hand_over(encode(tile, params))[:, :, None, :]

    return jax.shard_map(local_forward, mesh=mesh, in_specs=(act_spec,) + (P(),) * 12, out_specs=act_spec, check_vma=False)
```
